512 devices in a mesh: real: 2 (over y), env: 32 (over z), mpo: 4 (over x), col: 2 (over core).
Axes of the slice: x: 4, y: 2, z: 32, core: 2. Of those that a mesh axis runs over, the one named last changes fastest.
The devices are a block of a 4x8x32 slice.
Arguments:
- held: bfloat16 [24576, 8, 384], P(('real', 'env', 'col')), parts along dimension 0, may hold values from -0.15625 to 0.15625
- owner_map: int32 [64, 192], P('real'), parts along dimension 0, may hold values from 0 to 12287, as said below
- kept: int32 [64], P(('real', 'env')), parts along dimension 0, may hold values from 96 to 384
- left_env: bfloat16 [16, 64, 384, 384], P('mpo', ('real', 'env')), parts along dimension 1, may hold values from -6 to 6
- mpo_tensor: float32 [14, 14, 4, 4], replicated, may hold values from -1 to 1
- mpo_mask: int32 [14, 14], replicated, may hold values 0 or 1
- fields: float32 [4], P('real'), parts along dimension 0, may hold values from -2 to 2
Outputs:
- new_env: float32 [16, 64, 384, 384], P('mpo', ('real', 'env'), None, 'col'), parts along dimension 1
The draws below stay inside these ranges and needn't reach their ends.
There are 2 independent parts, one for each index of `real`. The reference program is written for one: setup_inputs(seed, part) draws one part's arguments, and reference() takes and returns one part's arrays. A program takes and returns all parts, laid end to end along the dimension named above; an argument that names none is the same for every part. Nothing has to cross between parts.
Inputs may be any that keep to these rules, and one draw needn't show every extreme that they name: owner_map[t, j] is the slot of held that holds tile j of sector t; all entries differ. The owner of index o along env+col holds the slots o * 192 to (o + 1) * 192 - 1. Among the tiles of one sector (the sector of one env index), one owner holds at most 6, and for every sector some owner holds exactly 6.
All inputs are finite; a program needn't handle non-finite values.
Results may differ from the reference program's by a relative error of at most 0.0042.
Values may be sent and summed in bfloat16 or wider, within the bound.
No kernel may reach another device: no remote copies, remote signals or barrier semaphores. Data moves between devices by JAX's collectives and lax.ppermute only.
A program may use at most 64 MiB of HBM per device.

```python
import jax
import jax.numpy as jnp
from jax import lax

P_SIZE = 4
K = 14
B = 384
TILE = 8
SEC_DEV = 1
S = 32
NT = 192
CAP = 6
POOL = 192
SLOTS = 12288
KSL = 4
KP = 16
N_MPO = 4


def draw_owner_map(key, part):
    owners = 2 * SEC_DEV * NT // CAP
    row_count = S // SEC_DEV
    tiles_row = SEC_DEV * NT
    heavy = jax.random.randint(jax.random.fold_in(key, 11), (owners,), 0, 4)
    order = jax.vmap(lambda sub: jax.random.permutation(sub, POOL))(jax.random.split(jax.random.fold_in(key, 12), owners))

    def one_row(row):
        row_key = jax.random.fold_in(jax.random.fold_in(key, 13), row)
        candidate = jnp.arange(owners * CAP, dtype=jnp.int32)
        cand_owner = candidate // CAP
        noise = jax.random.randint(jax.random.fold_in(row_key, 1), (owners * CAP,), 0, 4096)
        forced = jax.random.randint(jax.random.fold_in(row_key, 2), (), 0, owners)
        score = noise + heavy[cand_owner] * 2048 + jnp.where(cand_owner == forced, 32768, 0)
        score = score * (owners * CAP) + candidate
        unused, chosen = lax.top_k(score, tiles_row)
        chosen = jax.random.permutation(jax.random.fold_in(row_key, 3), chosen)
        chosen_owner = chosen // CAP
        chosen_rank = chosen % CAP
        position = order[chosen_owner, row * CAP + chosen_rank]
        return chosen_owner * POOL + position
    table = jax.vmap(one_row)(jnp.arange(row_count, dtype=jnp.int32))
    return table.reshape(S, NT).astype(jnp.int32)


def with_ends(drawn, key, least, largest):
    longest = drawn.shape.index(max(drawn.shape))
    spots = []
    for shift in (0, 1):
        where = [jax.random.randint(jax.random.fold_in(key, axis), (), 0, length) for axis, length in enumerate(drawn.shape)]
        where[longest] = (where[longest] + shift) % drawn.shape[longest]
        spots.append(tuple(where))
    return drawn.at[spots[0]].set(least).at[spots[1]].set(largest)


def block_scale(stream_key, shape, shards, smallest, top_value):
    factor_of = 1.0
    for axis_at, blocks in shards:
        steps = jax.random.uniform(jax.random.fold_in(jax.random.fold_in(stream_key, 6), axis_at), (blocks,), jnp.float32, smallest / len(shards), top_value / len(shards))
        factor_of = factor_of * jnp.repeat(jnp.exp(steps), shape[axis_at] // blocks).reshape((-1,) + (1,) * (len(shape) - 1 - axis_at))
    return factor_of


def bell_draw(own_key, dims, width, limit, pieces=(), held_as=jnp.bfloat16):
    drawn = width * jax.random.normal(own_key, dims, jnp.float32)
    if pieces:
        drawn = drawn * block_scale(own_key, dims, pieces, -0.22, 0.18)
    return jnp.clip(drawn, -limit, limit).astype(held_as)


def setup_inputs(seed: int = 0, part: int = 0) -> dict:
    splits = jax.random.split(jax.random.key(seed), 8)
    own_keys = jax.random.split(jax.random.fold_in(splits[7], part), 8)
    return {
        "held": bell_draw(own_keys[0], (SLOTS, TILE, B), (P_SIZE * B) ** -0.5, 0.15625, ((0, 64),)),
        "owner_map": draw_owner_map(jax.random.fold_in(jax.random.fold_in(splits[7], part), 71), part),
        "kept": with_ends(jax.random.randint(own_keys[2], (S,), B // 4, B + 1), jax.random.fold_in(own_keys[2], 1), B // 4, B).astype(jnp.int32),
        "left_env": bell_draw(own_keys[3], (KP, S, B, B), 1.0, 6.0, ((0, 4), (1, 32))),
        "mpo_tensor": bell_draw(splits[4], (K, K, P_SIZE, P_SIZE), (K * P_SIZE // 2) ** -0.5, 1.0, (), jnp.float32),
        "mpo_mask": with_ends((jax.random.randint(splits[5], (K, K), 0, 2) < 1).astype(jnp.int32), jax.random.fold_in(splits[5], 1), 0, 1),
        "fields": jnp.clip(jax.random.uniform(own_keys[6], (2,), jnp.float32, -2.0, 2.0), -2.0, 2.0),
    }


def build_couplings(mpo_tensor, mpo_mask, fields, padded):
    bond = mpo_tensor.shape[0]
    states = mpo_tensor.shape[2]
    base = mpo_tensor * mpo_mask.astype(jnp.float32)[:, :, None, None]
    level = jnp.arange(states, dtype=jnp.int32)
    spin_first = 0.5 - (level // 2).astype(jnp.float32)
    spin_second = 0.5 - (level % 2).astype(jnp.float32)
    onsite = jnp.diag(fields[0] * spin_first + fields[1] * spin_second)
    bond_index = jnp.arange(bond, dtype=jnp.int32)
    corner = (bond_index[:, None] == bond - 1) & (bond_index[None, :] == 0)
    base = base + jnp.where(corner[:, :, None, None], onsite[None, None, :, :], jnp.float32(0.0))
    return jnp.pad(base, ((0, padded - bond), (0, padded - bond), (0, 0), (0, 0)))


def reference(held, owner_map, kept, left_env, mpo_tensor, mpo_mask, fields):
    tiles = jnp.take(held, owner_map.reshape(-1), axis=0)
    sector_matrices = tiles.reshape(S, P_SIZE, B, B)
    columns = jnp.arange(B, dtype=jnp.int32)
    keep = columns[None, :] < kept[:, None]
    sector_matrices = jnp.where(keep[:, None, None, :], sector_matrices, jnp.zeros((), jnp.bfloat16))
    couplings = build_couplings(mpo_tensor, mpo_mask, fields, KP)
    leading_sector = lax.Precision.HIGHEST

    def one_sector(pair):
        block, environment = pair
        bond_vectors = block.astype(jnp.float32)
        first = jnp.einsum("wij,sja->wsia", environment[:K].astype(jnp.float32), bond_vectors, precision=leading_sector)
        contracted_sum = jnp.zeros((K, P_SIZE, B, B), jnp.float32)
        for slab_index in range(N_MPO):
            lower = slab_index * KSL
            upper = min(lower + KSL, K)
            if lower < K:
                next_spin = jnp.einsum("wvts,wsia->vtia", couplings[lower:upper, :K], first[lower:upper], precision=leading_sector)
                rounded = lax.optimization_barrier(next_spin.astype(jnp.bfloat16))
                contracted_sum = contracted_sum + rounded.astype(jnp.float32)
        updated_environment = jnp.einsum("hze,shzo->seo", bond_vectors, contracted_sum, precision=leading_sector)
        return jnp.pad(updated_environment, ((0, KP - K), (0, 0), (0, 0)))

    stacked = lax.map(one_sector, (sector_matrices, jnp.moveaxis(left_env, 1, 0)))
    return jnp.moveaxis(stacked, 0, 1)
```

```python
import functools

import jax
import jax.numpy as jnp
from jax import lax
from jax.experimental import pallas as pl
from jax.experimental.pallas import tpu as pltpu
from jax.sharding import PartitionSpec as P


F32 = jnp.float32
BF16 = jnp.bfloat16
CHUNKS = 2
PLANES = 4


def iota(shape, dim):
    return lax.broadcasted_iota(jnp.int32, shape, dim)


def onehot(condition):
    return jnp.where(condition, F32(1.0), F32(0.0)).astype(BF16)


def dot(a, b):
    return lax.dot_general(a, b, (((1,), (0,)), ((), ())), preferred_element_type=F32)


def dot_t(a, b):
    return lax.dot_general(a, b, (((1,), (1,)), ((), ())), preferred_element_type=F32)


def vmem(n):
    return [pl.BlockSpec(memory_space=pltpu.VMEM)] * n


SMEM = pl.BlockSpec(memory_space=pltpu.SMEM)


def pack_kernel(capacity, tile, rows, ids_ref, map_ref, held_ref, out_ref, spread_ref):
    me, plane = ids_ref[0], ids_ref[1]
    sectors, tiles = map_ref.shape
    count, width = held_ref.shape
    pool = count // tile
    blocks = width // 128
    local = map_ref[...] - me * pool
    mine = (local >= 0) & (local < pool)
    upto = onehot(iota((tiles, tiles), 0) <= iota((tiles, tiles), 1))
    rank = dot(onehot(mine), upto)
    slots = jnp.zeros((sectors, 128), F32)
    lane = iota((sectors, 128), 1)
    for s in range(capacity):
        hit = mine & (rank == F32(s + 1))
        value = jnp.sum(jnp.where(hit, local, 0).astype(F32), axis=1, keepdims=True)
        slots = slots + jnp.where(lane == s, value, F32(0.0))
    group = capacity * rows
    message = blocks * group
    total = sectors * group
    inner = iota((total, 1), 0) % group
    sector = iota((total, sectors), 0) // group
    spread = dot(onehot(sector == iota((total, sectors), 1)), slots.astype(BF16))
    slot = jnp.sum(jnp.where(iota((total, 128), 1) == inner // rows, spread, F32(0.0)), axis=1, keepdims=True)
    source = slot.astype(jnp.int32) * tile + plane * rows + inner % rows
    result = dot(onehot(source == iota((total, count), 1)), held_ref[...])
    for t in range(sectors):
        for b in range(blocks):
            at = t * message + b * group
            spread_ref[at : at + group, :] = result[t * group : (t + 1) * group, b * 128 : (b + 1) * 128]
    out_ref[...] = spread_ref[...].astype(BF16)


def unpack_kernel(capacity, pool, cores, rows, ids_ref, map_ref, own_ref, peer_ref, out_ref):
    core = ids_ref[2]
    tiles = map_ref.shape[1]
    width = out_ref.shape[1]
    blocks = width // 128
    group = capacity * rows
    message = blocks * group
    owner_row = jnp.broadcast_to(map_ref[...], (tiles, tiles)) // pool
    eye = iota((tiles, tiles), 0) == iota((tiles, tiles), 1)
    owner = jnp.sum(jnp.where(eye, owner_row, 0).astype(F32), axis=1, keepdims=True).astype(jnp.int32)
    before = (owner == owner_row) & (iota((tiles, tiles), 1) < iota((tiles, tiles), 0))
    rank = jnp.sum(jnp.where(before, F32(1.0), F32(0.0)), axis=1, keepdims=True).astype(jnp.int32)
    place = (owner // cores) * message + rank * rows + core
    own = jnp.where(owner % cores == core, place, -2 * message)
    peer = jnp.where(owner % cores == core, -2 * message, place)
    column = iota((tiles, own_ref.shape[0]), 1)
    for b in range(blocks):
        value = dot(onehot(column == own + b * group), own_ref[...])
        value = value + dot(onehot(column == peer + b * group), peer_ref[...])
        out_ref[:, b * 128 : (b + 1) * 128] = value.astype(BF16)


def fold_kernel(ids_ref, fields_ref, tensor_ref, mask_ref, own_ref, *rest):
    out_ref, weight_ref = rest[-2:]
    got = rest[: PLANES - 1]
    planes = PLANES
    plane = ids_ref[1]
    slab, step_rows, width = own_ref.shape
    slots = planes * slab
    states = out_ref.shape[2] // width
    pairs = out_ref.shape[0]
    cols = slots * states * states
    half = step_rows // 2
    rows = pairs * half
    total = states * rows
    deep = slots * half

    @pl.when(pl.program_id(0) == 0)
    def _():
        mask = mask_ref[...].astype(BF16)
        lanes_v = onehot(iota((slots, cols), 1) // (states * states) == iota((slots, cols), 0))
        base = tensor_ref[...] * dot(mask, lanes_v)
        w = iota((slots, cols), 0)
        lane = iota((slots, cols), 1)
        q, s = lane // states, lane % states
        first = F32(0.5) - (s // 2).astype(F32)
        second = F32(0.5) - (s % 2).astype(F32)
        onsite = fields_ref[0] * first + fields_ref[1] * second
        bond = ids_ref[3]
        base = base + jnp.where((w == bond - 1) & (q == s) & (lane < states * states), onsite, F32(0.0))
        high = base.astype(BF16)
        low = (base - high.astype(F32)).astype(BF16)
        row = iota((total, cols), 0)
        pair = (row // half) % pairs
        state = row // rows
        wanted = (plane * (pairs // states) + pair // states) * (states * states) + (pair % states) * states + state
        choose = onehot(wanted == iota((total, cols), 1))
        rel = iota((slots, deep), 1) // half
        absolute = ((plane - rel // slab + planes) % planes) * slab + rel % slab
        widen = onehot(absolute == iota((slots, deep), 0))
        diagonal = iota((total, deep), 0) % half == iota((total, deep), 1) % half
        for part, value in ((0, high), (1, low)):
            tall = dot_t(choose, value).astype(BF16)
            weight_ref[:, part * deep : (part + 1) * deep] = jnp.where(diagonal, dot(tall, widen), F32(0.0)).astype(BF16)

    env = jnp.concatenate([r[...] for r in (own_ref, *got)], axis=0).astype(F32)
    parts = []
    for h in range(2):
        part = env[:, h * half : (h + 1) * half, :].reshape(deep, width).astype(BF16)
        parts.append(jnp.concatenate([part, part], axis=0))
    for s in range(states):
        weight = weight_ref[s * rows : (s + 1) * rows, :]
        value = [dot(weight, part).reshape(pairs, half, width) for part in parts]
        out_ref[:, :, s * width : (s + 1) * width] = jnp.concatenate(value, axis=1).astype(BF16)


def apply_kernel(tile, ids_ref, kept_ref, *refs):
    pieces = refs[: 2 * PLANES]
    fold_ref, out_ref, ordered, natural, own, turned = refs[2 * PLANES :]
    plane, core = ids_ref[1], ids_ref[2]
    tiles, width = pieces[0].shape
    states = tiles * tile // width
    planes = len(pieces) // 2
    per_state = tiles // states
    share = own.shape[1]
    q = pl.program_id(1)

    @pl.when((pl.program_id(0) == 0) & (q == 0))
    def _():
        keep = iota((tiles, width), 1) < kept_ref[0]
        for d in range(planes):
            for other in range(2):
                r = ((plane - d + planes) % planes) * 2 + (core + other) % 2
                ordered[r] = jnp.where(keep, pieces[d * 2 + other][...], jnp.zeros((), BF16))
        n, k = iota((width, width), 0), iota((width, width), 1)
        turn = onehot((n % tile) * per_state + n // tile == k)
        for s in range(states):
            mixed = ordered[:, s * per_state : (s + 1) * per_state, :].reshape(width, width)
            value = dot(turn, mixed)
            rows = slice(s * width, (s + 1) * width)
            natural[rows, :] = value.astype(BF16)
            own[rows, :] = jnp.where(core == 0, value[:, :share], value[:, share:]).astype(BF16)

    mid = dot(fold_ref[0], own[...])
    turned[q] = jnp.swapaxes(mid, 0, 1).astype(BF16)

    @pl.when(q == states - 1)
    def _():
        total = dot(turned[0], natural[0:width, :])
        for s in range(1, states):
            total = total + dot(turned[s], natural[s * width : (s + 1) * width, :])
        out_ref[0, 0] = total


def fold(ids, fields, tensor, mask, own, got, half, chunk, previous, states):
    slab, width, _ = own.shape
    planes = len(got) + 1
    pairs = slab * states
    step = 16
    steps = got[0].shape[1] // step
    half_steps = width // 2 // step
    fixed = lambda shape: pl.BlockSpec(shape, lambda i, ids: (0,) * len(shape))
    at = lambda i, ids: ((ids[2] + half) % 2) * half_steps + chunk * steps + i
    in_specs = [
        SMEM,
        fixed(tensor.shape),
        fixed(mask.shape),
        pl.BlockSpec((slab, step, width), lambda i, ids: (0, at(i, ids), 0)),
    ] + [pl.BlockSpec((slab, step, width), lambda i, ids: (0, i, 0))] * len(got)
    args = [ids, fields, tensor, mask, own, *got]
    alias = {}
    if previous is not None:
        in_specs.append(pl.BlockSpec(memory_space=pl.ANY))
        alias = {len(args): 0}
        args.append(previous)
    slots = planes * slab
    return pl.pallas_call(
        fold_kernel,
        grid_spec=pltpu.PrefetchScalarGridSpec(
            num_scalar_prefetch=1,
            grid=(steps,),
            in_specs=in_specs,
            out_specs=pl.BlockSpec((pairs, step, states * width), lambda i, ids: (0, at(i, ids), 0)),
            scratch_shapes=[pltpu.VMEM((states * pairs * step // 2, slots * step), BF16)],
        ),
        out_shape=jax.ShapeDtypeStruct((pairs, width, states * width), BF16),
        input_output_aliases=alias,
        cost_estimate=pl.CostEstimate(flops=2 * steps * 1024 * 256 * width, bytes_accessed=6 << 20, transcendentals=0),
    )(*args)


def on_device(held, owner_map, kept, left_env, mpo_tensor, mpo_mask, fields):
    env_count = lax.axis_size("env")
    cores = lax.axis_size("col")
    planes = lax.axis_size("mpo")
    env_row = lax.axis_index("env")
    core = lax.axis_index("col")
    plane = lax.axis_index("mpo")
    pool, tile, width = held.shape
    tiles = owner_map.shape[1]
    states = tiles * tile // width
    capacity = 2 * tiles // (env_count * cores)
    rows = tile // planes
    slab = left_env.shape[0]
    slots = slab * planes
    bond = mpo_tensor.shape[0]
    ids = jnp.stack([env_row * cores + core, plane, core, jnp.int32(bond)]).astype(jnp.int32)

    def shift(x, axis, d):
        n = lax.axis_size(axis)
        return lax.ppermute(x, axis, [(i, (i + d) % n) for i in range(n)])

    env_own = left_env[:, 0]
    share_rows = width // cores
    piece_rows = share_rows // CHUNKS
    env_got, env_other = [], []
    for chunk in range(CHUNKS):
        part = lax.dynamic_slice_in_dim(env_own, core * share_rows + chunk * piece_rows, piece_rows, 1)
        env_got.append([shift(part, "mpo", d) for d in (1, 3, 2)])
        env_got[-1] = [env_got[-1][0], env_got[-1][2], env_got[-1][1]]
        env_other.append([shift(x, "col", 1) for x in env_got[-1]])

    message = rows * capacity * width // 128
    packed = pl.pallas_call(
        functools.partial(pack_kernel, capacity, tile, rows),
        in_specs=[SMEM] + vmem(2),
        out_specs=pl.BlockSpec(memory_space=pltpu.VMEM),
        out_shape=jax.ShapeDtypeStruct((env_count * message, 128), BF16),
        scratch_shapes=[pltpu.VMEM((env_count * message, 128), F32)],
        cost_estimate=pl.CostEstimate(flops=2 * 1536 * 1152 * 384, bytes_accessed=2 << 20, transcendentals=0),
        name="pack",
    )(ids, owner_map, held.reshape(pool * tile, width))
    arrived = lax.all_to_all(packed.reshape(env_count, message // 4, 4, 128), "env", 0, 0, tiled=True)

    tensor = jnp.pad(mpo_tensor.reshape(bond, bond * states * states), ((0, slots - bond), (0, (slots - bond) * states * states)))
    mask = jnp.pad(mpo_mask.astype(F32), ((0, slots - bond), (0, slots - bond)))
    folded = None
    for chunk in range(CHUNKS):
        for half, got in ((0, env_got[chunk]), (1, env_other[chunk])):
            folded = fold(ids, fields, tensor, mask, env_own, got, half, chunk, folded, states)

    map_here = lax.dynamic_slice_in_dim(owner_map, env_row, 1, 0)
    arrived = arrived.reshape(env_count * message, 128)
    swapped = shift(arrived, "col", 1)
    mine = pl.pallas_call(
        functools.partial(unpack_kernel, capacity, pool, cores, rows),
        in_specs=[SMEM] + vmem(3),
        out_specs=pl.BlockSpec(memory_space=pltpu.VMEM),
        out_shape=jax.ShapeDtypeStruct((tiles, width), BF16),
        cost_estimate=pl.CostEstimate(flops=2 * 384 * 1152 * 384, bytes_accessed=1 << 20, transcendentals=0),
        name="unpack",
    )(ids, map_here, arrived, swapped)
    by_plane = [mine]
    for d in range(1, planes):
        by_plane.append(shift(mine, "mpo", d))
    pieces = []
    for piece in by_plane:
        pieces += [piece, shift(piece, "col", 1)]

    share = width // cores
    result = pl.pallas_call(
        functools.partial(apply_kernel, tile),
        grid_spec=pltpu.PrefetchScalarGridSpec(
            num_scalar_prefetch=2,
            grid=(slab, states),
            in_specs=[pl.BlockSpec((tiles, width), lambda v, q, *_: (0, 0))] * (2 * planes)
            + [pl.BlockSpec((1, width, states * width), lambda v, q, *_: (v * states + q, 0, 0))],
            out_specs=pl.BlockSpec((1, 1, share, width), lambda v, q, *_: (v, 0, 0, 0)),
            scratch_shapes=[
                pltpu.VMEM((tile, tiles, width), BF16),
                pltpu.VMEM((states * width, width), BF16),
                pltpu.VMEM((states * width, share), BF16),
                pltpu.VMEM((states, share, width), BF16),
            ],
        ),
        out_shape=jax.ShapeDtypeStruct((slab, 1, share, width), F32),
        cost_estimate=pl.CostEstimate(flops=9 << 29, bytes_accessed=22 << 20, transcendentals=0),
        name="apply",
    )(ids, kept, *pieces, folded)
    return jnp.swapaxes(result, 2, 3)


def solution(mesh):
    return jax.shard_map(
        on_device,
        mesh=mesh,
        in_specs=(
            P(("real", "env", "col"), None, None),
            P("real", None),
            P(("real", "env")),
            P("mpo", ("real", "env"), None, None),
            P(),
            P(),
            P("real"),
        ),
        out_specs=P("mpo", ("real", "env"), None, "col"),
        check_vma=False,
    )
```

```python
import functools

import jax
import jax.numpy as jnp
from jax import lax
from jax.experimental import pallas as pl
from jax.experimental.pallas import tpu as pltpu
from jax.sharding import PartitionSpec as P


F32 = jnp.float32
BF16 = jnp.bfloat16


def iota(shape, dim):
    return lax.broadcasted_iota(jnp.int32, shape, dim)


def onehot(condition):
    return jnp.where(condition, F32(1.0), F32(0.0)).astype(BF16)


def dot(a, b):
    return lax.dot_general(a, b, (((1,), (0,)), ((), ())), preferred_element_type=F32)


def dot_t(a, b):
    return lax.dot_general(a, b, (((1,), (1,)), ((), ())), preferred_element_type=F32)


def vmem(n):
    return [pl.BlockSpec(memory_space=pltpu.VMEM)] * n


SMEM = pl.BlockSpec(memory_space=pltpu.SMEM)


def pack_kernel(capacity, tile, rows, ids_ref, map_ref, held_ref, out_ref, spread_ref):
    me, plane = ids_ref[0], ids_ref[1]
    sectors, tiles = map_ref.shape
    count, width = held_ref.shape
    pool = count // tile
    blocks = width // 128
    local = map_ref[...] - me * pool
    mine = (local >= 0) & (local < pool)
    upto = onehot(iota((tiles, tiles), 0) <= iota((tiles, tiles), 1))
    rank = dot(onehot(mine), upto)
    slots = jnp.zeros((sectors, 128), F32)
    lane = iota((sectors, 128), 1)
    for s in range(capacity):
        hit = mine & (rank == F32(s + 1))
        value = jnp.sum(jnp.where(hit, local, 0).astype(F32), axis=1, keepdims=True)
        slots = slots + jnp.where(lane == s, value, F32(0.0))
    group = capacity * rows
    message = blocks * group
    total = sectors * group
    inner = iota((total, 1), 0) % group
    sector = iota((total, sectors), 0) // group
    spread = dot(onehot(sector == iota((total, sectors), 1)), slots.astype(BF16))
    slot = jnp.sum(jnp.where(iota((total, 128), 1) == inner // rows, spread, F32(0.0)), axis=1, keepdims=True)
    source = slot.astype(jnp.int32) * tile + plane * rows + inner % rows
    result = dot(onehot(source == iota((total, count), 1)), held_ref[...])
    for t in range(sectors):
        for b in range(blocks):
            at = t * message + b * group
            spread_ref[at : at + group, :] = result[t * group : (t + 1) * group, b * 128 : (b + 1) * 128]
    out_ref[...] = spread_ref[...].astype(BF16)


def unpack_kernel(capacity, pool, cores, rows, ids_ref, map_ref, own_ref, peer_ref, out_ref):
    core = ids_ref[2]
    tiles = map_ref.shape[1]
    width = out_ref.shape[1]
    blocks = width // 128
    group = capacity * rows
    message = blocks * group
    owner_row = jnp.broadcast_to(map_ref[...], (tiles, tiles)) // pool
    eye = iota((tiles, tiles), 0) == iota((tiles, tiles), 1)
    owner = jnp.sum(jnp.where(eye, owner_row, 0).astype(F32), axis=1, keepdims=True).astype(jnp.int32)
    before = (owner == owner_row) & (iota((tiles, tiles), 1) < iota((tiles, tiles), 0))
    rank = jnp.sum(jnp.where(before, F32(1.0), F32(0.0)), axis=1, keepdims=True).astype(jnp.int32)
    place = (owner // cores) * message + rank * rows + core
    own = jnp.where(owner % cores == core, place, -2 * message)
    peer = jnp.where(owner % cores == core, -2 * message, place)
    column = iota((tiles, own_ref.shape[0]), 1)
    for b in range(blocks):
        value = dot(onehot(column == own + b * group), own_ref[...])
        value = value + dot(onehot(column == peer + b * group), peer_ref[...])
        out_ref[:, b * 128 : (b + 1) * 128] = value.astype(BF16)


def fold_kernel(ids_ref, fields_ref, tensor_ref, mask_ref, own_ref, got_ref, out_ref, weight_ref):
    plane = ids_ref[1]
    slab, step_rows, width = own_ref.shape
    slots = slab + got_ref.shape[0]
    planes = slots // slab
    states = out_ref.shape[2] // width
    pairs = out_ref.shape[0]
    cols = slots * states * states
    half = 8
    rows = pairs * half
    total = states * rows
    deep = slots * half

    @pl.when(pl.program_id(0) == 0)
    def _():
        mask = mask_ref[...].astype(BF16)
        lanes_v = onehot(iota((slots, cols), 1) // (states * states) == iota((slots, cols), 0))
        base = tensor_ref[...] * dot(mask, lanes_v)
        w = iota((slots, cols), 0)
        lane = iota((slots, cols), 1)
        q, s = lane // states, lane % states
        first = F32(0.5) - (s // 2).astype(F32)
        second = F32(0.5) - (s % 2).astype(F32)
        onsite = fields_ref[0] * first + fields_ref[1] * second
        bond = ids_ref[3]
        base = base + jnp.where((w == bond - 1) & (q == s) & (lane < states * states), onsite, F32(0.0))
        high = base.astype(BF16)
        low = (base - high.astype(F32)).astype(BF16)
        row = iota((total, cols), 0)
        pair = (row // half) % pairs
        state = row // rows
        wanted = (plane * (pairs // states) + pair // states) * (states * states) + (pair % states) * states + state
        choose = onehot(wanted == iota((total, cols), 1))
        slot = iota((slots, deep), 1) // half
        slot = (plane - slot // slab + planes) % planes * slab + slot % slab
        widen = onehot(slot == iota((slots, deep), 0))
        diagonal = iota((total, deep), 0) % half == iota((total, deep), 1) % half
        for part, value in ((0, high), (1, low)):
            tall = dot_t(choose, value).astype(BF16)
            weight_ref[:, part * deep : (part + 1) * deep] = jnp.where(diagonal, dot(tall, widen), F32(0.0)).astype(BF16)

    for at in range(0, step_rows, 16):
        env = jnp.concatenate([own_ref[:, at : at + 16, :], got_ref[:, at : at + 16, :]], axis=0).astype(F32)
        side = jnp.concatenate([env[:, h * half : (h + 1) * half, :].reshape(deep, width) for h in range(2)], axis=1)
        side = side.astype(BF16)
        value = dot(weight_ref[...], jnp.concatenate([side, side], axis=0))
        for s in range(states):
            part = [
                value[s * rows : (s + 1) * rows, h * width : (h + 1) * width].reshape(pairs, half, width)
                for h in range(2)
            ]
            out_ref[:, at : at + 16, s * width : (s + 1) * width] = jnp.concatenate(part, axis=1).astype(BF16)


def apply_kernel(tile, ids_ref, kept_ref, mine_ref, twin_ref, near_ref, far_ref, out_ref, ordered, halves, own, turned):
    core = ids_ref[2]
    planes, tiles, width = mine_ref.shape
    states = tiles * tile // width
    per_state = tiles // states
    share = own.shape[1]

    @pl.when(pl.program_id(0) == 0)
    def _():
        keep = iota((tiles, width), 1) < kept_ref[0]
        for p in range(planes):
            for other, ref in ((0, mine_ref), (1, twin_ref)):
                ordered[p * 2 + (core + other) % 2] = jnp.where(keep, ref[p], jnp.zeros((), BF16))
        n, k = iota((width, width), 0), iota((width, width), 1)
        turn = onehot((n % tile) * per_state + n // tile == k)
        for s in range(states):
            mixed = ordered[:, s * per_state : (s + 1) * per_state, :].reshape(width, width)
            value = dot(turn, mixed)
            own[s * width : (s + 1) * width, :] = jnp.where(core == 0, value[:, :share], value[:, share:]).astype(BF16)
            first = pl.multiple_of(s * width + core * share, share)
            second = pl.multiple_of(s * width + (1 - core) * share, share)
            halves[pl.ds(first, share), :] = value[:share].astype(BF16)
            halves[pl.ds(second, share), :] = value[share:].astype(BF16)

    for q in range(states):
        mid = dot(jnp.concatenate([near_ref[q], far_ref[q]], axis=0), own[...])
        turned[:, q * width : (q + 1) * width] = jnp.swapaxes(mid, 0, 1).astype(BF16)
    out_ref[0, 0] = dot(turned[...], halves[...])


def fold(ids, fields, tensor, mask, own, got, half, states):
    others, count, width = got.shape
    slab = own.shape[0]
    slots, pairs = slab + others, slab * states
    step = 48
    steps = count // step
    fixed = lambda shape: pl.BlockSpec(shape, lambda i, ids: (0,) * len(shape))
    return pl.pallas_call(
        fold_kernel,
        grid_spec=pltpu.PrefetchScalarGridSpec(
            num_scalar_prefetch=1,
            grid=(steps,),
            in_specs=[
                SMEM,
                fixed(tensor.shape),
                fixed(mask.shape),
                pl.BlockSpec((slab, step, width), lambda i, ids: (0, ((ids[2] + half) % 2) * steps + i, 0)),
                pl.BlockSpec((others, step, width), lambda i, ids: (0, i, 0)),
            ],
            out_specs=pl.BlockSpec((pairs, step, states * width), lambda i, ids: (0, i, 0)),
            scratch_shapes=[pltpu.VMEM((states * pairs * 8, slots * 16), BF16)],
        ),
        out_shape=jax.ShapeDtypeStruct((pairs, count, states * width), BF16),
        cost_estimate=pl.CostEstimate(flops=2 * steps * 1024 * 256 * width, bytes_accessed=12 << 20, transcendentals=0),
    )(ids, fields, tensor, mask, own, got)


def call_pack(ids, owner_map, held, capacity, tile, rows):
    sectors, width = owner_map.shape[0], held.shape[1]
    count = sectors * rows * capacity * width // 128
    return pl.pallas_call(
        functools.partial(pack_kernel, capacity, tile, rows),
        in_specs=[SMEM] + vmem(2),
        out_specs=pl.BlockSpec(memory_space=pltpu.VMEM),
        out_shape=jax.ShapeDtypeStruct((count, 128), BF16),
        scratch_shapes=[pltpu.VMEM((count, 128), F32)],
        cost_estimate=pl.CostEstimate(flops=1 << 29, bytes_accessed=2 << 20, transcendentals=0),
        name="pack",
    )(ids, owner_map, held)


def call_unpack(ids, map_here, arrived, swapped, capacity, pool, cores, rows):
    tiles = map_here.shape[1]
    width = arrived.size // (tiles * rows)
    return pl.pallas_call(
        functools.partial(unpack_kernel, capacity, pool, cores, rows),
        in_specs=[SMEM] + vmem(3),
        out_specs=pl.BlockSpec(memory_space=pltpu.VMEM),
        out_shape=jax.ShapeDtypeStruct((tiles, width), BF16),
        cost_estimate=pl.CostEstimate(flops=2 * 384 * 1152 * 384, bytes_accessed=1 << 20, transcendentals=0),
        name="unpack",
    )(ids, map_here, arrived, swapped)


def call_apply(ids, kept, by_plane, by_twin, near, far, tile):
    planes, tiles, width = by_plane.shape
    pairs, share, deep = near.shape
    states = deep // width
    slab = pairs // states
    whole = lambda v, *_: (0, 0, 0)
    return pl.pallas_call(
        functools.partial(apply_kernel, tile),
        grid_spec=pltpu.PrefetchScalarGridSpec(
            num_scalar_prefetch=2,
            grid=(slab,),
            in_specs=[pl.BlockSpec((planes, tiles, width), whole)] * 2
            + [pl.BlockSpec((states, share, deep), lambda v, *_: (v, 0, 0))] * 2,
            out_specs=pl.BlockSpec((1, 1, share, width), lambda v, *_: (v, 0, 0, 0)),
            scratch_shapes=[
                pltpu.VMEM((tile, tiles, width), BF16),
                pltpu.VMEM((deep, width), BF16),
                pltpu.VMEM((deep, share), BF16),
                pltpu.VMEM((share, deep), BF16),
            ],
        ),
        out_shape=jax.ShapeDtypeStruct((slab, 1, share, width), F32),
        cost_estimate=pl.CostEstimate(flops=9 << 29, bytes_accessed=22 << 20, transcendentals=0),
        name="apply",
    )(ids, kept, by_plane, by_twin, near, far)


def on_device(held, owner_map, kept, left_env, mpo_tensor, mpo_mask, fields):
    env_count = lax.axis_size("env")
    cores = lax.axis_size("col")
    planes = lax.axis_size("mpo")
    env_row = lax.axis_index("env")
    core = lax.axis_index("col")
    plane = lax.axis_index("mpo")
    pool, tile, width = held.shape
    tiles = owner_map.shape[1]
    states = tiles * tile // width
    capacity = 2 * tiles // (env_count * cores)
    rows = tile // planes
    slab = left_env.shape[0]
    slots = slab * planes
    bond = mpo_tensor.shape[0]
    ids = jnp.stack([env_row * cores + core, plane, core, jnp.int32(bond)]).astype(jnp.int32)

    def twin(x):
        return lax.ppermute(x, "col", [(0, 1), (1, 0)])

    def gather(x):
        return lax.all_to_all(jnp.broadcast_to(x, (planes, *x.shape)), "mpo", 0, 0, tiled=True)

    message = rows * capacity * width // 128
    packed = call_pack(ids, owner_map, held.reshape(pool * tile, width), capacity, tile, rows)
    arrived = lax.all_to_all(packed.reshape(env_count, message // 4, 4, 128), "env", 0, 0, tiled=True)

    share = width // cores
    env_own = left_env[:, 0]
    env_half = lax.dynamic_slice_in_dim(env_own, core * share, share, 1)
    step = lambda x, d: lax.ppermute(x, "mpo", [(i, (i + d) % planes) for i in range(planes)])
    from_left, from_right = step(env_half, 1), step(env_half, -1)
    ring = [(i * cores + c, (i + 1 - 2 * c) % planes * cores + c) for i in range(planes) for c in range(cores)]
    from_far = lax.ppermute(jnp.where(core == 0, from_left, from_right), ("mpo", "col"), ring)
    env_got = jnp.concatenate([from_left, from_far, from_right], axis=0)

    tensor = jnp.pad(
        mpo_tensor.reshape(bond, bond * states * states), ((0, slots - bond), (0, (slots - bond) * states * states))
    )
    mask = jnp.pad(mpo_mask.astype(F32), ((0, slots - bond), (0, slots - bond)))
    map_here = lax.dynamic_slice_in_dim(owner_map, env_row, 1, 0)
    env_got, tensor, mask, map_here = lax.optimization_barrier((env_got, tensor, mask, map_here))
    env_twin = twin(env_got)
    folded_mine = fold(ids, fields, tensor, mask, env_own, env_got, 0, states)
    folded_twin = fold(ids, fields, tensor, mask, env_own, env_twin, 1, states)

    arrived = arrived.reshape(env_count * message, 128)
    swapped = twin(arrived)
    mine = call_unpack(ids, map_here, arrived, swapped, capacity, pool, cores, rows)
    by_plane = gather(mine)
    by_twin = twin(by_plane)

    result = call_apply(ids, kept, by_plane, by_twin, folded_mine, folded_twin, tile)
    return jnp.swapaxes(result, 2, 3)


def solution(mesh):
    return jax.shard_map(
        on_device,
        mesh=mesh,
        in_specs=(
            P(("real", "env", "col"), None, None),
            P("real", None),
            P(("real", "env")),
            P("mpo", ("real", "env"), None, None),
            P(),
            P(),
            P("real"),
        ),
        out_specs=P("mpo", ("real", "env"), None, "col"),
        check_vma=False,
    )
```

```python
import functools

import jax
import jax.numpy as jnp
from jax import lax
from jax.experimental import pallas as pl
from jax.experimental.pallas import tpu as pltpu
from jax.sharding import PartitionSpec as P


F32 = jnp.float32
BF16 = jnp.bfloat16


GROUP = 8
CHUNKS = 2


def iota(shape, dim):
    return lax.broadcasted_iota(jnp.int32, shape, dim)


def onehot(condition):
    return jnp.where(condition, F32(1.0), F32(0.0)).astype(BF16)


def dot(a, b):
    return lax.dot_general(a, b, (((1,), (0,)), ((), ())), preferred_element_type=F32)


def dot_t(a, b):
    return lax.dot_general(a, b, (((1,), (1,)), ((), ())), preferred_element_type=F32)


def vmem(n):
    return [pl.BlockSpec(memory_space=pltpu.VMEM)] * n


SMEM = pl.BlockSpec(memory_space=pltpu.SMEM)


def pack_kernel(capacity, tile, rows, ids_ref, map_ref, held_ref, out_ref, spread_ref):
    me, plane = ids_ref[0], ids_ref[1]
    sectors, tiles = map_ref.shape
    count, width = held_ref.shape
    pool = count // tile
    blocks = width // 128
    local = map_ref[...] - me * pool
    mine = (local >= 0) & (local < pool)
    upto = onehot(iota((tiles, tiles), 0) <= iota((tiles, tiles), 1))
    rank = dot(onehot(mine), upto)
    slots = jnp.zeros((sectors, 128), F32)
    lane = iota((sectors, 128), 1)
    for s in range(capacity):
        hit = mine & (rank == F32(s + 1))
        value = jnp.sum(jnp.where(hit, local, 0).astype(F32), axis=1, keepdims=True)
        slots = slots + jnp.where(lane == s, value, F32(0.0))
    group = capacity * rows
    message = blocks * group
    total = sectors * group
    inner = iota((total, 1), 0) % group
    sector = iota((total, sectors), 0) // group
    spread = dot(onehot(sector == iota((total, sectors), 1)), slots.astype(BF16))
    slot = jnp.sum(jnp.where(iota((total, 128), 1) == inner // rows, spread, F32(0.0)), axis=1, keepdims=True)
    source = slot.astype(jnp.int32) * tile + plane * rows + inner % rows
    result = dot(onehot(source == iota((total, count), 1)), held_ref[...])
    for t in range(sectors):
        for b in range(blocks):
            at = t * message + b * group
            spread_ref[at : at + group, :] = result[t * group : (t + 1) * group, b * 128 : (b + 1) * 128]
    out_ref[...] = spread_ref[...].astype(BF16)


def unpack_kernel(capacity, pool, cores, rows, ids_ref, map_ref, own_ref, peer_ref, out_ref):
    core = ids_ref[2]
    tiles = map_ref.shape[1]
    width = out_ref.shape[2]
    blocks = width // 128
    group = capacity * rows
    message = blocks * group
    owner_row = jnp.broadcast_to(map_ref[...], (tiles, tiles)) // pool
    eye = iota((tiles, tiles), 0) == iota((tiles, tiles), 1)
    owner = jnp.sum(jnp.where(eye, owner_row, 0).astype(F32), axis=1, keepdims=True).astype(jnp.int32)
    before = (owner == owner_row) & (iota((tiles, tiles), 1) < iota((tiles, tiles), 0))
    rank = jnp.sum(jnp.where(before, F32(1.0), F32(0.0)), axis=1, keepdims=True).astype(jnp.int32)
    place = (owner // cores) * message + rank * rows + core
    own = jnp.where(owner % cores == core, place, -2 * message)
    peer = jnp.where(owner % cores == core, -2 * message, place)
    column = iota((tiles, own_ref.shape[0]), 1)
    for b in range(blocks):
        value = dot(onehot(column == own + b * group), own_ref[...])
        value = value + dot(onehot(column == peer + b * group), peer_ref[...])
        for copy in range(out_ref.shape[0]):
            out_ref[copy, :, b * 128 : (b + 1) * 128] = value.astype(BF16)


def weight_kernel(slab, states, group, ids_ref, fields_ref, tensor_ref, mask_ref, out_ref):
    plane = ids_ref[1]
    slots, cols = tensor_ref.shape
    planes = slots // slab
    pairs = slab * states
    rows = pairs * group
    total = states * rows
    deep = slots * group
    mask = mask_ref[...].astype(BF16)
    lanes_v = onehot(iota((slots, cols), 1) // (states * states) == iota((slots, cols), 0))
    base = tensor_ref[...] * dot(mask, lanes_v)
    w = iota((slots, cols), 0)
    lane = iota((slots, cols), 1)
    q, s = lane // states, lane % states
    first = F32(0.5) - (s // 2).astype(F32)
    second = F32(0.5) - (s % 2).astype(F32)
    onsite = fields_ref[0] * first + fields_ref[1] * second
    base = base + jnp.where((w == ids_ref[3] - 1) & (q == s) & (lane < states * states), onsite, F32(0.0))
    high = base.astype(BF16)
    low = (base - high.astype(F32)).astype(BF16)
    row = iota((total, cols), 0)
    pair = (row // group) % pairs
    state = row // rows
    wanted = (plane * slab + pair // states) * (states * states) + (pair % states) * states + state
    choose = onehot(wanted == iota((total, cols), 1))
    slot = iota((slots, deep), 1) // group
    slot = (plane - slot // slab + planes) % planes * slab + slot % slab
    widen = onehot(slot == iota((slots, deep), 0))
    diagonal = iota((total, deep), 0) % group == iota((total, deep), 1) % group
    for part, value in ((0, high), (1, low)):
        tall = dot_t(choose, value).astype(BF16)
        out_ref[:, part * deep : (part + 1) * deep] = jnp.where(diagonal, dot(tall, widen), F32(0.0)).astype(BF16)


def call_weights(ids, fields, tensor, mask, slab, states):
    slots = tensor.shape[0]
    return pl.pallas_call(
        functools.partial(weight_kernel, slab, states, GROUP),
        in_specs=[SMEM] * 2 + vmem(2),
        out_specs=pl.BlockSpec(memory_space=pltpu.VMEM),
        out_shape=jax.ShapeDtypeStruct((states * slab * states * GROUP, 2 * slots * GROUP), BF16),
        cost_estimate=pl.CostEstimate(flops=1 << 28, bytes_accessed=1 << 19, transcendentals=0),
        name="weights",
    )(ids, fields, tensor, mask)


def fold_kernel(ids_ref, weight_ref, own_ref, got_ref, out_ref):
    slab, step_rows, width = own_ref.shape
    slots = slab + got_ref.shape[0]
    states = out_ref.shape[2] // width
    pairs = out_ref.shape[0]
    rows = pairs * GROUP
    for at in range(0, step_rows, 2 * GROUP):
        here = slice(at, at + 2 * GROUP)
        env = jnp.concatenate([own_ref[:, here, :], got_ref[:, here, :]], axis=0).astype(F32)
        side = [env[:, h * GROUP : (h + 1) * GROUP, :].reshape(slots * GROUP, width) for h in range(2)]
        side = jnp.concatenate(side, axis=1).astype(BF16)
        value = dot(weight_ref[...], jnp.concatenate([side, side], axis=0))
        for s in range(states):
            part = [
                value[s * rows : (s + 1) * rows, h * width : (h + 1) * width].reshape(pairs, GROUP, width)
                for h in range(2)
            ]
            out_ref[:, here, s * width : (s + 1) * width] = jnp.concatenate(part, axis=1).astype(BF16)


def apply_kernel(tile, ids_ref, kept_ref, mine_ref, twin_ref, *refs):
    folded = refs[: 2 * CHUNKS]
    out_ref, ordered, halves, own, turned = refs[2 * CHUNKS :]
    core = ids_ref[2]
    planes, tiles, width = mine_ref.shape
    states = tiles * tile // width
    per_state = tiles // states
    share = own.shape[1]

    @pl.when(pl.program_id(0) == 0)
    def _():
        keep = iota((tiles, width), 1) < kept_ref[0]
        for p in range(planes):
            for other, ref in ((0, mine_ref), (1, twin_ref)):
                ordered[p * 2 + (core + other) % 2] = jnp.where(keep, ref[p], jnp.zeros((), BF16))
        n, k = iota((width, width), 0), iota((width, width), 1)
        turn = onehot((n % tile) * per_state + n // tile == k)
        for s in range(states):
            mixed = ordered[:, s * per_state : (s + 1) * per_state, :].reshape(width, width)
            value = dot(turn, mixed)
            own[s * width : (s + 1) * width, :] = jnp.where(core == 0, value[:, :share], value[:, share:]).astype(BF16)
            first = pl.multiple_of(s * width + core * share, share)
            second = pl.multiple_of(s * width + (1 - core) * share, share)
            halves[pl.ds(first, share), :] = value[:share].astype(BF16)
            halves[pl.ds(second, share), :] = value[share:].astype(BF16)

    for q in range(states):
        mid = dot(jnp.concatenate([ref[q] for ref in folded], axis=0), own[...])
        turned[:, q * width : (q + 1) * width] = jnp.swapaxes(mid, 0, 1).astype(BF16)
    out_ref[0, 0] = dot(turned[...], halves[...])


def fold(ids, weights, own, got, half, chunk, states):
    others, count, width = got.shape
    slab = own.shape[0]
    pairs = slab * states
    step = 48
    steps = count // step
    return pl.pallas_call(
        fold_kernel,
        grid_spec=pltpu.PrefetchScalarGridSpec(
            num_scalar_prefetch=1,
            grid=(steps,),
            in_specs=[
                pl.BlockSpec(weights.shape, lambda i, ids: (0, 0)),
                pl.BlockSpec(
                    (slab, step, width), lambda i, ids: (0, ((ids[2] + half) % 2 * CHUNKS + chunk) * steps + i, 0)
                ),
                pl.BlockSpec((others, step, width), lambda i, ids: (0, i, 0)),
            ],
            out_specs=pl.BlockSpec((pairs, step, states * width), lambda i, ids: (0, i, 0)),
        ),
        out_shape=jax.ShapeDtypeStruct((pairs, count, states * width), BF16),
        cost_estimate=pl.CostEstimate(flops=2 * count * 64 * 256 * width, bytes_accessed=6 << 20, transcendentals=0),
    )(ids, weights, own, got)


def call_pack(ids, owner_map, held, capacity, tile, rows):
    sectors, width = owner_map.shape[0], held.shape[1]
    count = sectors * rows * capacity * width // 128
    return pl.pallas_call(
        functools.partial(pack_kernel, capacity, tile, rows),
        in_specs=[SMEM] + vmem(2),
        out_specs=pl.BlockSpec(memory_space=pltpu.VMEM),
        out_shape=jax.ShapeDtypeStruct((count, 128), BF16),
        scratch_shapes=[pltpu.VMEM((count, 128), F32)],
        cost_estimate=pl.CostEstimate(flops=1 << 29, bytes_accessed=2 << 20, transcendentals=0),
        name="pack",
    )(ids, owner_map, held)


def call_unpack(ids, map_here, arrived, swapped, capacity, pool, cores, rows, copies):
    tiles = map_here.shape[1]
    width = arrived.size // (tiles * rows)
    return pl.pallas_call(
        functools.partial(unpack_kernel, capacity, pool, cores, rows),
        in_specs=[SMEM] + vmem(3),
        out_specs=pl.BlockSpec(memory_space=pltpu.VMEM),
        out_shape=jax.ShapeDtypeStruct((copies, tiles, width), BF16),
        cost_estimate=pl.CostEstimate(flops=2 * 384 * 1152 * 384, bytes_accessed=1 << 20, transcendentals=0),
        compiler_params=pltpu.CompilerParams(vmem_limit_bytes=16 << 20),
        name="unpack",
    )(ids, map_here, arrived, swapped)


def call_apply(ids, kept, by_plane, by_twin, folded, tile):
    planes, tiles, width = by_plane.shape
    pairs, part, deep = folded[0].shape
    share = width // 2
    states = deep // width
    slab = pairs // states
    whole = lambda v, *_: (0, 0, 0)
    return pl.pallas_call(
        functools.partial(apply_kernel, tile),
        grid_spec=pltpu.PrefetchScalarGridSpec(
            num_scalar_prefetch=2,
            grid=(slab,),
            in_specs=[pl.BlockSpec((planes, tiles, width), whole)] * 2
            + [pl.BlockSpec((states, part, deep), lambda v, *_: (v, 0, 0))] * len(folded),
            out_specs=pl.BlockSpec((1, 1, share, width), lambda v, *_: (v, 0, 0, 0)),
            scratch_shapes=[
                pltpu.VMEM((tile, tiles, width), BF16),
                pltpu.VMEM((deep, width), BF16),
                pltpu.VMEM((deep, share), BF16),
                pltpu.VMEM((share, deep), BF16),
            ],
        ),
        out_shape=jax.ShapeDtypeStruct((slab, 1, share, width), F32),
        cost_estimate=pl.CostEstimate(flops=9 << 29, bytes_accessed=22 << 20, transcendentals=0),
        name="apply",
    )(ids, kept, by_plane, by_twin, *folded)


def on_device(held, owner_map, kept, left_env, mpo_tensor, mpo_mask, fields):
    env_count = lax.axis_size("env")
    cores = lax.axis_size("col")
    planes = lax.axis_size("mpo")
    env_row = lax.axis_index("env")
    core = lax.axis_index("col")
    plane = lax.axis_index("mpo")
    pool, tile, width = held.shape
    tiles = owner_map.shape[1]
    states = tiles * tile // width
    capacity = 2 * tiles // (env_count * cores)
    rows = tile // planes
    slab = left_env.shape[0]
    slots = slab * planes
    bond = mpo_tensor.shape[0]
    ids = jnp.stack([env_row * cores + core, plane, core, jnp.int32(bond)]).astype(jnp.int32)

    def twin(x):
        return lax.ppermute(x, "col", [(0, 1), (1, 0)])

    message = rows * capacity * width // 128
    packed = call_pack(ids, owner_map, held.reshape(pool * tile, width), capacity, tile, rows)
    arrived = lax.all_to_all(packed.reshape(env_count, message // 4, 4, 128), "env", 0, 0, tiled=True)

    share = width // cores
    env_own = left_env[:, 0]
    step = lambda x, d: lax.ppermute(x, "mpo", [(i, (i + d) % planes) for i in range(planes)])
    ring = [(i * cores + c, (i + 1 - 2 * c) % planes * cores + c) for i in range(planes) for c in range(cores)]
    chunk_rows = share // CHUNKS
    env_got = []
    for chunk in range(CHUNKS):
        part = lax.dynamic_slice_in_dim(env_own, core * share + chunk * chunk_rows, chunk_rows, 1)
        from_left, from_right = step(part, 1), step(part, -1)
        from_far = lax.ppermute(jnp.where(core == 0, from_left, from_right), ("mpo", "col"), ring)
        env_got.append(jnp.concatenate([from_left, from_far, from_right], axis=0))

    tensor = jnp.pad(
        mpo_tensor.reshape(bond, bond * states * states), ((0, slots - bond), (0, (slots - bond) * states * states))
    )
    mask = jnp.pad(mpo_mask.astype(F32), ((0, slots - bond), (0, slots - bond)))
    weights = call_weights(ids, fields, tensor, mask, slab, states)
    map_here = lax.dynamic_slice_in_dim(owner_map, env_row, 1, 0)
    env_got[0], weights, map_here = lax.optimization_barrier((env_got[0], weights, map_here))
    folded = [None] * (2 * CHUNKS)
    for chunk in range(CHUNKS):
        env_twin = twin(env_got[chunk])
        for half, got in ((0, env_got[chunk]), (1, env_twin)):
            folded[half * CHUNKS + chunk] = fold(ids, weights, env_own, got, half, chunk, states)

    arrived = arrived.reshape(env_count * message, 128)
    swapped = twin(arrived)
    mine = call_unpack(ids, map_here, arrived, swapped, capacity, pool, cores, rows, planes)
    by_plane = lax.all_to_all(mine, "mpo", 0, 0, tiled=True)
    by_twin = twin(by_plane)

    result = call_apply(ids, kept, by_plane, by_twin, folded, tile)
    return jnp.swapaxes(result, 2, 3)


def solution(mesh):
    return jax.shard_map(
        on_device,
        mesh=mesh,
        in_specs=(
            P(("real", "env", "col"), None, None),
            P("real", None),
            P(("real", "env")),
            P("mpo", ("real", "env"), None, None),
            P(),
            P(),
            P("real"),
        ),
        out_specs=P("mpo", ("real", "env"), None, "col"),
        check_vma=False,
    )
```

```python
import functools

import jax
import jax.numpy as jnp
from jax import lax
from jax.experimental import pallas as pl
from jax.experimental.pallas import tpu as pltpu
from jax.sharding import PartitionSpec as P


F32 = jnp.float32
BF16 = jnp.bfloat16


GROUP = 8
CHUNKS = 1


def iota(shape, dim):
    return lax.broadcasted_iota(jnp.int32, shape, dim)


def onehot(condition):
    return jnp.where(condition, F32(1.0), F32(0.0)).astype(BF16)


def dot(a, b):
    return lax.dot_general(a, b, (((1,), (0,)), ((), ())), preferred_element_type=F32)


def dot_t(a, b):
    return lax.dot_general(a, b, (((1,), (1,)), ((), ())), preferred_element_type=F32)


def vmem(n):
    return [pl.BlockSpec(memory_space=pltpu.VMEM)] * n


SMEM = pl.BlockSpec(memory_space=pltpu.SMEM)


def pack_kernel(capacity, tile, rows, ids_ref, map_ref, held_ref, out_ref, spread_ref):
    me, plane = ids_ref[0], ids_ref[1]
    sectors, tiles = map_ref.shape
    count, width = held_ref.shape
    pool = count // tile
    blocks = width // 128
    local = map_ref[...] - me * pool
    mine = (local >= 0) & (local < pool)
    upto = onehot(iota((tiles, tiles), 0) <= iota((tiles, tiles), 1))
    rank = dot(onehot(mine), upto)
    slots = jnp.zeros((sectors, 128), F32)
    lane = iota((sectors, 128), 1)
    for s in range(capacity):
        hit = mine & (rank == F32(s + 1))
        value = jnp.sum(jnp.where(hit, local, 0).astype(F32), axis=1, keepdims=True)
        slots = slots + jnp.where(lane == s, value, F32(0.0))
    group = capacity * rows
    total = sectors * group
    inner = iota((total, 1), 0) % group
    sector = iota((total, sectors), 0) // group
    spread = dot(onehot(sector == iota((total, sectors), 1)), slots.astype(BF16))
    slot = jnp.sum(jnp.where(iota((total, 128), 1) == inner % capacity, spread, F32(0.0)), axis=1, keepdims=True)
    source = slot.astype(jnp.int32) * tile + plane * rows + inner // capacity
    result = dot(onehot(source == iota((total, count), 1)), held_ref[...])
    for t in range(sectors * rows):
        for b in range(blocks):
            at = (t * blocks + b) * capacity
            spread_ref[at : at + capacity, :] = result[t * capacity : (t + 1) * capacity, b * 128 : (b + 1) * 128]
    out_ref[...] = spread_ref[...].astype(BF16)


def unpack_kernel(capacity, pool, map_ref, got_ref, out_ref):
    tiles = map_ref.shape[1]
    width = out_ref.shape[2]
    blocks = width // 128
    owner_row = jnp.broadcast_to(map_ref[...], (tiles, tiles)) // pool
    eye = iota((tiles, tiles), 0) == iota((tiles, tiles), 1)
    owner = jnp.sum(jnp.where(eye, owner_row, 0).astype(F32), axis=1, keepdims=True).astype(jnp.int32)
    before = (owner == owner_row) & (iota((tiles, tiles), 1) < iota((tiles, tiles), 0))
    rank = jnp.sum(jnp.where(before, F32(1.0), F32(0.0)), axis=1, keepdims=True).astype(jnp.int32)
    place = owner * (blocks * capacity) + rank
    column = iota((tiles, got_ref.shape[0]), 1)
    for b in range(blocks):
        value = dot(onehot(column == place + b * capacity), got_ref[...]).astype(BF16)
        for copy in range(out_ref.shape[0]):
            out_ref[copy, :, b * 128 : (b + 1) * 128] = value


def weight_kernel(slab, states, group, ids_ref, fields_ref, tensor_ref, mask_ref, out_ref):
    plane = ids_ref[1]
    slots, cols = tensor_ref.shape
    planes = slots // slab
    pairs = slab * states
    rows = pairs * group
    total = states * rows
    deep = slots * group
    mask = mask_ref[...].astype(BF16)
    lanes_v = onehot(iota((slots, cols), 1) // (states * states) == iota((slots, cols), 0))
    base = tensor_ref[...] * dot(mask, lanes_v)
    w = iota((slots, cols), 0)
    lane = iota((slots, cols), 1)
    q, s = lane // states, lane % states
    first = F32(0.5) - (s // 2).astype(F32)
    second = F32(0.5) - (s % 2).astype(F32)
    onsite = fields_ref[0] * first + fields_ref[1] * second
    base = base + jnp.where((w == ids_ref[3] - 1) & (q == s) & (lane < states * states), onsite, F32(0.0))
    high = base.astype(BF16)
    low = (base - high.astype(F32)).astype(BF16)
    row = iota((total, cols), 0)
    pair = (row // group) % pairs
    state = row // rows
    wanted = (plane * slab + pair // states) * (states * states) + (pair % states) * states + state
    choose = onehot(wanted == iota((total, cols), 1))
    slot = iota((slots, deep), 1) // group
    slot = (plane - slot // slab + planes) % planes * slab + slot % slab
    widen = onehot(slot == iota((slots, deep), 0))
    diagonal = iota((total, deep), 0) % group == iota((total, deep), 1) % group
    for part, value in ((0, high), (1, low)):
        tall = dot_t(choose, value).astype(BF16)
        out_ref[:, part * deep : (part + 1) * deep] = jnp.where(diagonal, dot(tall, widen), F32(0.0)).astype(BF16)


def call_weights(ids, fields, tensor, mask, slab, states):
    slots = tensor.shape[0]
    return pl.pallas_call(
        functools.partial(weight_kernel, slab, states, GROUP),
        in_specs=[SMEM] * 2 + vmem(2),
        out_specs=pl.BlockSpec(memory_space=pltpu.VMEM),
        out_shape=jax.ShapeDtypeStruct((states * slab * states * GROUP, 2 * slots * GROUP), BF16),
        cost_estimate=pl.CostEstimate(flops=1 << 28, bytes_accessed=1 << 19, transcendentals=0),
        name="weights",
    )(ids, fields, tensor, mask)


def fold_kernel(ids_ref, weight_ref, own_ref, got_ref, out_ref):
    slab, step_rows, width = own_ref.shape
    slots = slab + got_ref.shape[0]
    states = out_ref.shape[2] // width
    pairs = out_ref.shape[0]
    rows = pairs * GROUP
    for at in range(0, step_rows, 2 * GROUP):
        here = slice(at, at + 2 * GROUP)
        env = jnp.concatenate([own_ref[:, here, :], got_ref[:, here, :]], axis=0).astype(F32)
        side = [env[:, h * GROUP : (h + 1) * GROUP, :].reshape(slots * GROUP, width) for h in range(2)]
        side = jnp.concatenate(side, axis=1).astype(BF16)
        value = dot(weight_ref[...], jnp.concatenate([side, side], axis=0))
        for s in range(states):
            part = [
                value[s * rows : (s + 1) * rows, h * width : (h + 1) * width].reshape(pairs, GROUP, width)
                for h in range(2)
            ]
            out_ref[:, here, s * width : (s + 1) * width] = jnp.concatenate(part, axis=1).astype(BF16)


def apply_kernel(tile, ids_ref, kept_ref, rows_ref, *refs):
    folded = refs[: 2 * CHUNKS]
    out_ref, halves, own, turned = refs[2 * CHUNKS :]
    core = ids_ref[2]
    _, tiles, width = rows_ref.shape
    states = tiles * tile // width
    per_state = tiles // states
    share = own.shape[1]

    @pl.when(pl.program_id(0) == 0)
    def _():
        keep = iota((width, width), 1) < kept_ref[0]
        n, k = iota((width, width), 0), iota((width, width), 1)
        turn = onehot((n % tile) * per_state + n // tile == k)
        for s in range(states):
            mixed = rows_ref[:, s * per_state : (s + 1) * per_state, :].reshape(width, width)
            value = jnp.where(keep, dot(turn, mixed), F32(0.0))
            own[s * width : (s + 1) * width, :] = jnp.where(core == 0, value[:, :share], value[:, share:]).astype(BF16)
            first = pl.multiple_of(s * width + core * share, share)
            second = pl.multiple_of(s * width + (1 - core) * share, share)
            halves[pl.ds(first, share), :] = value[:share].astype(BF16)
            halves[pl.ds(second, share), :] = value[share:].astype(BF16)

    for q in range(states):
        mid = dot(jnp.concatenate([ref[q] for ref in folded], axis=0), own[...])
        turned[:, q * width : (q + 1) * width] = jnp.swapaxes(mid, 0, 1).astype(BF16)
    out_ref[0, 0] = dot(turned[...], halves[...])


def fold(ids, weights, own, got, half, chunk, states):
    others, count, width = got.shape
    slab = own.shape[0]
    pairs = slab * states
    step = 48
    steps = count // step
    return pl.pallas_call(
        fold_kernel,
        grid_spec=pltpu.PrefetchScalarGridSpec(
            num_scalar_prefetch=1,
            grid=(steps,),
            in_specs=[
                pl.BlockSpec(weights.shape, lambda i, ids: (0, 0)),
                pl.BlockSpec(
                    (slab, step, width), lambda i, ids: (0, ((ids[2] + half) % 2 * CHUNKS + chunk) * steps + i, 0)
                ),
                pl.BlockSpec((others, step, width), lambda i, ids: (0, i, 0)),
            ],
            out_specs=pl.BlockSpec((pairs, step, states * width), lambda i, ids: (0, i, 0)),
        ),
        out_shape=jax.ShapeDtypeStruct((pairs, count, states * width), BF16),
        cost_estimate=pl.CostEstimate(flops=2 * count * 64 * 256 * width, bytes_accessed=6 << 20, transcendentals=0),
    )(ids, weights, own, got)


def call_pack(ids, owner_map, held, capacity, tile, rows):
    sectors, width = owner_map.shape[0], held.shape[1]
    count = sectors * rows * capacity * width // 128
    return pl.pallas_call(
        functools.partial(pack_kernel, capacity, tile, rows),
        in_specs=[SMEM] + vmem(2),
        out_specs=pl.BlockSpec(memory_space=pltpu.VMEM),
        out_shape=jax.ShapeDtypeStruct((count, 128), BF16),
        scratch_shapes=[pltpu.VMEM((count, 128), F32)],
        cost_estimate=pl.CostEstimate(flops=1 << 29, bytes_accessed=2 << 20, transcendentals=0),
        name="pack",
    )(ids, owner_map, held)


def call_unpack(map_here, arrived, capacity, pool, copies):
    tiles = map_here.shape[1]
    width = arrived.size // tiles // 2
    return pl.pallas_call(
        functools.partial(unpack_kernel, capacity, pool),
        in_specs=vmem(2),
        out_specs=pl.BlockSpec(memory_space=pltpu.VMEM),
        out_shape=jax.ShapeDtypeStruct((copies, tiles, width), BF16),
        cost_estimate=pl.CostEstimate(flops=1 << 28, bytes_accessed=2 << 20, transcendentals=0),
        compiler_params=pltpu.CompilerParams(vmem_limit_bytes=16 << 20),
        name="unpack",
    )(map_here, arrived)


def call_apply(ids, kept, rows, folded, tile):
    _, tiles, width = rows.shape
    pairs, part, deep = folded[0].shape
    share = width // 2
    states = deep // width
    slab = pairs // states
    whole = lambda v, *_: (0, 0, 0)
    return pl.pallas_call(
        functools.partial(apply_kernel, tile),
        grid_spec=pltpu.PrefetchScalarGridSpec(
            num_scalar_prefetch=2,
            grid=(slab,),
            in_specs=[pl.BlockSpec((tile, tiles, width), whole)]
            + [pl.BlockSpec((states, part, deep), lambda v, *_: (v, 0, 0))] * len(folded),
            out_specs=pl.BlockSpec((1, 1, share, width), lambda v, *_: (v, 0, 0, 0)),
            scratch_shapes=[
                pltpu.VMEM((deep, width), BF16),
                pltpu.VMEM((deep, share), BF16),
                pltpu.VMEM((share, deep), BF16),
            ],
        ),
        out_shape=jax.ShapeDtypeStruct((slab, 1, share, width), F32),
        cost_estimate=pl.CostEstimate(flops=9 << 29, bytes_accessed=22 << 20, transcendentals=0),
        name="apply",
    )(ids, kept, rows, *folded)


def on_device(held, owner_map, kept, left_env, mpo_tensor, mpo_mask, fields):
    env_count = lax.axis_size("env")
    cores = lax.axis_size("col")
    planes = lax.axis_size("mpo")
    env_row = lax.axis_index("env")
    core = lax.axis_index("col")
    plane = lax.axis_index("mpo")
    pool, tile, width = held.shape
    tiles = owner_map.shape[1]
    states = tiles * tile // width
    capacity = 2 * tiles // (env_count * cores)
    rows = tile // planes
    slab = left_env.shape[0]
    slots = slab * planes
    bond = mpo_tensor.shape[0]
    ids = jnp.stack([env_row * cores + core, plane, core, jnp.int32(bond)]).astype(jnp.int32)

    def twin(x):
        return lax.ppermute(x, "col", [(0, 1), (1, 0)])

    members = env_count * cores
    message = capacity * width // 128
    packed = call_pack(ids, owner_map, held.reshape(pool * tile, width), capacity, tile, rows)
    arrived = lax.all_to_all(packed.reshape(members, message // 2, 2, 128), ("env", "col"), 0, 0, tiled=True)

    share = width // cores
    env_own = left_env[:, 0]
    step = lambda x, d: lax.ppermute(x, "mpo", [(i, (i + d) % planes) for i in range(planes)])
    ring = [(i * cores + c, (i + 1 - 2 * c) % planes * cores + c) for i in range(planes) for c in range(cores)]
    part = lax.dynamic_slice_in_dim(env_own, core * share, share, 1)
    from_left, from_right = step(part, 1), step(part, -1)
    tensor = jnp.pad(
        mpo_tensor.reshape(bond, bond * states * states), ((0, slots - bond), (0, (slots - bond) * states * states))
    )
    mask = jnp.pad(mpo_mask.astype(F32), ((0, slots - bond), (0, slots - bond)))
    weights = call_weights(ids, fields, tensor, mask, slab, states)
    map_here = lax.dynamic_slice_in_dim(owner_map, env_row, 1, 0)
    onward = jnp.where(core == 0, from_left, from_right)
    onward, weights, map_here = lax.optimization_barrier((onward, weights, map_here))
    from_far = lax.ppermute(onward, ("mpo", "col"), ring)
    env_got = jnp.concatenate([from_left, from_far, from_right], axis=0)
    env_twin = twin(env_got)
    folded = []
    for half, got in ((0, env_got), (1, env_twin)):
        folded.append(fold(ids, weights, env_own, got, half, 0, states))

    mine = call_unpack(map_here, arrived.reshape(members * message, 128), capacity, pool, planes * cores)
    tile_rows = lax.all_to_all(mine, ("mpo", "col"), 0, 0, tiled=True)
    result = call_apply(ids, kept, tile_rows, folded, tile)
    return jnp.swapaxes(result, 2, 3)


def solution(mesh):
    return jax.shard_map(
        on_device,
        mesh=mesh,
        in_specs=(
            P(("real", "env", "col"), None, None),
            P("real", None),
            P(("real", "env")),
            P("mpo", ("real", "env"), None, None),
            P(),
            P(),
            P("real"),
        ),
        out_specs=P("mpo", ("real", "env"), None, "col"),
        check_vma=False,
    )
```

```python
import functools

import jax
import jax.numpy as jnp
from jax import lax
from jax.experimental import pallas as pl
from jax.experimental.pallas import tpu as pltpu
from jax.sharding import PartitionSpec as P


F32 = jnp.float32
BF16 = jnp.bfloat16


GROUP = 8
CHUNKS = 1


def iota(shape, dim):
    return lax.broadcasted_iota(jnp.int32, shape, dim)


def onehot(condition):
    return jnp.where(condition, F32(1.0), F32(0.0)).astype(BF16)


def dot(a, b):
    return lax.dot_general(a, b, (((1,), (0,)), ((), ())), preferred_element_type=F32)


def dot_t(a, b):
    return lax.dot_general(a, b, (((1,), (1,)), ((), ())), preferred_element_type=F32)


def vmem(n):
    return [pl.BlockSpec(memory_space=pltpu.VMEM)] * n


SMEM = pl.BlockSpec(memory_space=pltpu.SMEM)


def pack_kernel(capacity, tile, rows, ids_ref, map_ref, held_ref, out_ref, spread_ref):
    me, plane = ids_ref[0], ids_ref[1]
    sectors, tiles = map_ref.shape
    count, width = held_ref.shape
    pool = count // tile
    blocks = width // 128
    local = map_ref[...] - me * pool
    mine = (local >= 0) & (local < pool)
    upto = onehot(iota((tiles, tiles), 0) <= iota((tiles, tiles), 1))
    rank = dot(onehot(mine), upto)
    slots = jnp.zeros((sectors, 128), F32)
    lane = iota((sectors, 128), 1)
    for s in range(capacity):
        hit = mine & (rank == F32(s + 1))
        value = jnp.sum(jnp.where(hit, local, 0).astype(F32), axis=1, keepdims=True)
        slots = slots + jnp.where(lane == s, value, F32(0.0))
    group = capacity * rows
    total = sectors * group
    inner = iota((total, 1), 0) % group
    sector = iota((total, sectors), 0) // group
    spread = dot(onehot(sector == iota((total, sectors), 1)), slots.astype(BF16))
    slot = jnp.sum(jnp.where(iota((total, 128), 1) == inner % capacity, spread, F32(0.0)), axis=1, keepdims=True)
    source = slot.astype(jnp.int32) * tile + plane * rows + inner // capacity
    result = dot(onehot(source == iota((total, count), 1)), held_ref[...])
    for t in range(sectors * rows):
        for b in range(blocks):
            at = (t * blocks + b) * capacity
            spread_ref[at : at + capacity, :] = result[t * capacity : (t + 1) * capacity, b * 128 : (b + 1) * 128]
    out_ref[...] = spread_ref[...].astype(BF16)


def unpack_kernel(capacity, pool, cores, ids_ref, map_ref, own_ref, peer_ref, out_ref):
    core = ids_ref[2]
    tiles = map_ref.shape[1]
    width = out_ref.shape[2]
    blocks = width // 128
    owner_row = jnp.broadcast_to(map_ref[...], (tiles, tiles)) // pool
    eye = iota((tiles, tiles), 0) == iota((tiles, tiles), 1)
    owner = jnp.sum(jnp.where(eye, owner_row, 0).astype(F32), axis=1, keepdims=True).astype(jnp.int32)
    before = (owner == owner_row) & (iota((tiles, tiles), 1) < iota((tiles, tiles), 0))
    rank = jnp.sum(jnp.where(before, F32(1.0), F32(0.0)), axis=1, keepdims=True).astype(jnp.int32)
    place = (owner // cores * cores + core) * (blocks * capacity) + rank
    own = jnp.where(owner % cores == core, place, -own_ref.shape[0])
    peer = jnp.where(owner % cores == core, -own_ref.shape[0], place)
    column = iota((tiles, own_ref.shape[0]), 1)
    for b in range(blocks):
        value = dot(onehot(column == own + b * capacity), own_ref[...])
        value = value + dot(onehot(column == peer + b * capacity), peer_ref[...])
        for copy in range(out_ref.shape[0]):
            out_ref[copy, :, b * 128 : (b + 1) * 128] = value.astype(BF16)


def weight_kernel(slab, states, group, ids_ref, fields_ref, tensor_ref, mask_ref, out_ref):
    plane = ids_ref[1]
    slots, cols = tensor_ref.shape
    planes = slots // slab
    pairs = slab * states
    rows = pairs * group
    total = states * rows
    deep = slots * group
    mask = mask_ref[...].astype(BF16)
    lanes_v = onehot(iota((slots, cols), 1) // (states * states) == iota((slots, cols), 0))
    base = tensor_ref[...] * dot(mask, lanes_v)
    w = iota((slots, cols), 0)
    lane = iota((slots, cols), 1)
    q, s = lane // states, lane % states
    first = F32(0.5) - (s // 2).astype(F32)
    second = F32(0.5) - (s % 2).astype(F32)
    onsite = fields_ref[0] * first + fields_ref[1] * second
    base = base + jnp.where((w == ids_ref[3] - 1) & (q == s) & (lane < states * states), onsite, F32(0.0))
    high = base.astype(BF16)
    low = (base - high.astype(F32)).astype(BF16)
    row = iota((total, cols), 0)
    pair = (row // group) % pairs
    state = row // rows
    wanted = (plane * slab + pair // states) * (states * states) + (pair % states) * states + state
    choose = onehot(wanted == iota((total, cols), 1))
    slot = iota((slots, deep), 1) // group
    slot = (plane - slot // slab + planes) % planes * slab + slot % slab
    widen = onehot(slot == iota((slots, deep), 0))
    diagonal = iota((total, deep), 0) % group == iota((total, deep), 1) % group
    for part, value in ((0, high), (1, low)):
        tall = dot_t(choose, value).astype(BF16)
        out_ref[:, part * deep : (part + 1) * deep] = jnp.where(diagonal, dot(tall, widen), F32(0.0)).astype(BF16)


def call_weights(ids, fields, tensor, mask, slab, states):
    slots = tensor.shape[0]
    return pl.pallas_call(
        functools.partial(weight_kernel, slab, states, GROUP),
        in_specs=[SMEM] * 2 + vmem(2),
        out_specs=pl.BlockSpec(memory_space=pltpu.VMEM),
        out_shape=jax.ShapeDtypeStruct((states * slab * states * GROUP, 2 * slots * GROUP), BF16),
        cost_estimate=pl.CostEstimate(flops=1 << 28, bytes_accessed=1 << 19, transcendentals=0),
        name="weights",
    )(ids, fields, tensor, mask)


def fold_kernel(ids_ref, weight_ref, own_ref, got_ref, out_ref):
    slab, step_rows, width = own_ref.shape
    slots = slab + got_ref.shape[0]
    states = out_ref.shape[2] // width
    pairs = out_ref.shape[0]
    rows = pairs * GROUP
    for at in range(0, step_rows, 2 * GROUP):
        here = slice(at, at + 2 * GROUP)
        env = jnp.concatenate([own_ref[:, here, :], got_ref[:, here, :]], axis=0).astype(F32)
        side = [env[:, h * GROUP : (h + 1) * GROUP, :].reshape(slots * GROUP, width) for h in range(2)]
        side = jnp.concatenate(side, axis=1).astype(BF16)
        value = dot(weight_ref[...], jnp.concatenate([side, side], axis=0))
        for s in range(states):
            part = [
                value[s * rows : (s + 1) * rows, h * width : (h + 1) * width].reshape(pairs, GROUP, width)
                for h in range(2)
            ]
            out_ref[:, here, s * width : (s + 1) * width] = jnp.concatenate(part, axis=1).astype(BF16)


def apply_kernel(tile, ids_ref, kept_ref, rows_ref, *refs):
    folded = refs[: 2 * CHUNKS]
    out_ref, halves, own, turned = refs[2 * CHUNKS :]
    core = ids_ref[2]
    _, tiles, width = rows_ref.shape
    states = tiles * tile // width
    per_state = tiles // states
    share = own.shape[1]

    @pl.when(pl.program_id(0) == 0)
    def _():
        keep = iota((width, width), 1) < kept_ref[0]
        n, k = iota((width, width), 0), iota((width, width), 1)
        turn = onehot((n % tile) * per_state + n // tile == k)
        for s in range(states):
            mixed = rows_ref[:, s * per_state : (s + 1) * per_state, :].reshape(width, width)
            value = jnp.where(keep, dot(turn, mixed), F32(0.0))
            own[s * width : (s + 1) * width, :] = jnp.where(core == 0, value[:, :share], value[:, share:]).astype(BF16)
            first = pl.multiple_of(s * width + core * share, share)
            second = pl.multiple_of(s * width + (1 - core) * share, share)
            halves[pl.ds(first, share), :] = value[:share].astype(BF16)
            halves[pl.ds(second, share), :] = value[share:].astype(BF16)

    for q in range(states):
        mid = dot(jnp.concatenate([ref[q] for ref in folded], axis=0), own[...])
        turned[:, q * width : (q + 1) * width] = jnp.swapaxes(mid, 0, 1).astype(BF16)
    out_ref[0, 0] = dot(turned[...], halves[...])


def fold(ids, weights, own, got, half, chunk, states):
    others, count, width = got.shape
    slab = own.shape[0]
    pairs = slab * states
    step = 48
    steps = count // step
    return pl.pallas_call(
        fold_kernel,
        grid_spec=pltpu.PrefetchScalarGridSpec(
            num_scalar_prefetch=1,
            grid=(steps,),
            in_specs=[
                pl.BlockSpec(weights.shape, lambda i, ids: (0, 0)),
                pl.BlockSpec(
                    (slab, step, width), lambda i, ids: (0, ((ids[2] + half) % 2 * CHUNKS + chunk) * steps + i, 0)
                ),
                pl.BlockSpec((others, step, width), lambda i, ids: (0, i, 0)),
            ],
            out_specs=pl.BlockSpec((pairs, step, states * width), lambda i, ids: (0, i, 0)),
        ),
        out_shape=jax.ShapeDtypeStruct((pairs, count, states * width), BF16),
        cost_estimate=pl.CostEstimate(flops=2 * count * 64 * 256 * width, bytes_accessed=6 << 20, transcendentals=0),
    )(ids, weights, own, got)


def call_pack(ids, owner_map, held, capacity, tile, rows):
    sectors, width = owner_map.shape[0], held.shape[1]
    count = sectors * rows * capacity * width // 128
    return pl.pallas_call(
        functools.partial(pack_kernel, capacity, tile, rows),
        in_specs=[SMEM] + vmem(2),
        out_specs=pl.BlockSpec(memory_space=pltpu.VMEM),
        out_shape=jax.ShapeDtypeStruct((count, 128), BF16),
        scratch_shapes=[pltpu.VMEM((count, 128), F32)],
        cost_estimate=pl.CostEstimate(flops=1 << 29, bytes_accessed=2 << 20, transcendentals=0),
        name="pack",
    )(ids, owner_map, held)


def call_unpack(ids, map_here, arrived, swapped, capacity, pool, cores, copies):
    tiles = map_here.shape[1]
    width = arrived.size // tiles // 2
    return pl.pallas_call(
        functools.partial(unpack_kernel, capacity, pool, cores),
        in_specs=[SMEM] + vmem(3),
        out_specs=pl.BlockSpec(memory_space=pltpu.VMEM),
        out_shape=jax.ShapeDtypeStruct((copies, tiles, width), BF16),
        cost_estimate=pl.CostEstimate(flops=1 << 28, bytes_accessed=2 << 20, transcendentals=0),
        compiler_params=pltpu.CompilerParams(vmem_limit_bytes=16 << 20),
        name="unpack",
    )(ids, map_here, arrived, swapped)


def call_apply(ids, kept, rows, folded, tile):
    _, tiles, width = rows.shape
    pairs, part, deep = folded[0].shape
    share = width // 2
    states = deep // width
    slab = pairs // states
    whole = lambda v, *_: (0, 0, 0)
    return pl.pallas_call(
        functools.partial(apply_kernel, tile),
        grid_spec=pltpu.PrefetchScalarGridSpec(
            num_scalar_prefetch=2,
            grid=(slab,),
            in_specs=[pl.BlockSpec((tile, tiles, width), whole)]
            + [pl.BlockSpec((states, part, deep), lambda v, *_: (v, 0, 0))] * len(folded),
            out_specs=pl.BlockSpec((1, 1, share, width), lambda v, *_: (v, 0, 0, 0)),
            scratch_shapes=[
                pltpu.VMEM((deep, width), BF16),
                pltpu.VMEM((deep, share), BF16),
                pltpu.VMEM((share, deep), BF16),
            ],
        ),
        out_shape=jax.ShapeDtypeStruct((slab, 1, share, width), F32),
        cost_estimate=pl.CostEstimate(flops=9 << 29, bytes_accessed=22 << 20, transcendentals=0),
        name="apply",
    )(ids, kept, rows, *folded)


def on_device(held, owner_map, kept, left_env, mpo_tensor, mpo_mask, fields):
    env_count = lax.axis_size("env")
    cores = lax.axis_size("col")
    planes = lax.axis_size("mpo")
    env_row = lax.axis_index("env")
    core = lax.axis_index("col")
    plane = lax.axis_index("mpo")
    pool, tile, width = held.shape
    tiles = owner_map.shape[1]
    states = tiles * tile // width
    capacity = 2 * tiles // (env_count * cores)
    rows = tile // planes
    slab = left_env.shape[0]
    slots = slab * planes
    bond = mpo_tensor.shape[0]
    ids = jnp.stack([env_row * cores + core, plane, core, jnp.int32(bond)]).astype(jnp.int32)

    def twin(x):
        return lax.ppermute(x, "col", [(0, 1), (1, 0)])

    message = rows * capacity * width // 128
    packed = call_pack(ids, owner_map, held.reshape(pool * tile, width), capacity, tile, rows)
    arrived = lax.all_to_all(packed.reshape(env_count, message // 4, 4, 128), "env", 0, 0, tiled=True)

    share = width // cores
    env_own = left_env[:, 0]
    step = lambda x, d: lax.ppermute(x, "mpo", [(i, (i + d) % planes) for i in range(planes)])
    ring = [(i * cores + c, (i + 1 - 2 * c) % planes * cores + c) for i in range(planes) for c in range(cores)]
    part = lax.dynamic_slice_in_dim(env_own, core * share, share, 1)
    from_left, from_right = step(part, 1), step(part, -1)
    tensor = jnp.pad(
        mpo_tensor.reshape(bond, bond * states * states), ((0, slots - bond), (0, (slots - bond) * states * states))
    )
    mask = jnp.pad(mpo_mask.astype(F32), ((0, slots - bond), (0, slots - bond)))
    weights = call_weights(ids, fields, tensor, mask, slab, states)
    map_here = lax.dynamic_slice_in_dim(owner_map, env_row, 1, 0)
    onward = jnp.where(core == 0, from_left, from_right)
    onward, weights, map_here = lax.optimization_barrier((onward, weights, map_here))
    from_far = lax.ppermute(onward, ("mpo", "col"), ring)
    env_got = jnp.concatenate([from_left, from_far, from_right], axis=0)
    env_twin = twin(env_got)
    folded = []
    for half, got in ((0, env_got), (1, env_twin)):
        folded.append(fold(ids, weights, env_own, got, half, 0, states))

    arrived = arrived.reshape(env_count * message, 128)
    swapped = twin(arrived)
    mine = call_unpack(ids, map_here, arrived, swapped, capacity, pool, cores, planes * cores)
    tile_rows = lax.all_to_all(mine, ("mpo", "col"), 0, 0, tiled=True)
    result = call_apply(ids, kept, tile_rows, folded, tile)
    return jnp.swapaxes(result, 2, 3)


def solution(mesh):
    return jax.shard_map(
        on_device,
        mesh=mesh,
        in_specs=(
            P(("real", "env", "col"), None, None),
            P("real", None),
            P(("real", "env")),
            P("mpo", ("real", "env"), None, None),
            P(),
            P(),
            P("real"),
        ),
        out_specs=P("mpo", ("real", "env"), None, "col"),
        check_vma=False,
    )
```

```python
import functools

import jax
import jax.numpy as jnp
from jax import lax
from jax.experimental import pallas as pl
from jax.experimental.pallas import tpu as pltpu
from jax.sharding import PartitionSpec as P


F32 = jnp.float32
BF16 = jnp.bfloat16


GROUP = 8
CHUNKS = 1


def iota(shape, dim):
    return lax.broadcasted_iota(jnp.int32, shape, dim)


def onehot(condition):
    return jnp.where(condition, F32(1.0), F32(0.0)).astype(BF16)


def dot(a, b):
    return lax.dot_general(a, b, (((1,), (0,)), ((), ())), preferred_element_type=F32)


def dot_t(a, b):
    return lax.dot_general(a, b, (((1,), (1,)), ((), ())), preferred_element_type=F32)


def vmem(n):
    return [pl.BlockSpec(memory_space=pltpu.VMEM)] * n


SMEM = pl.BlockSpec(memory_space=pltpu.SMEM)


def pack_kernel(capacity, tile, rows, ids_ref, map_ref, held_ref, out_ref, spread_ref):
    me, plane = ids_ref[0], ids_ref[1]
    sectors, tiles = map_ref.shape
    count, width = held_ref.shape
    pool = count // tile
    blocks = width // 128
    local = map_ref[...] - me * pool
    mine = (local >= 0) & (local < pool)
    upto = onehot(iota((tiles, tiles), 0) <= iota((tiles, tiles), 1))
    rank = dot(onehot(mine), upto)
    slots = jnp.zeros((sectors, 128), F32)
    lane = iota((sectors, 128), 1)
    for s in range(capacity):
        hit = mine & (rank == F32(s + 1))
        value = jnp.sum(jnp.where(hit, local, 0).astype(F32), axis=1, keepdims=True)
        slots = slots + jnp.where(lane == s, value, F32(0.0))
    group = capacity * rows
    total = sectors * group
    inner = iota((total, 1), 0) % group
    sector = iota((total, sectors), 0) // group
    spread = dot(onehot(sector == iota((total, sectors), 1)), slots.astype(BF16))
    slot = jnp.sum(jnp.where(iota((total, 128), 1) == inner % capacity, spread, F32(0.0)), axis=1, keepdims=True)
    source = slot.astype(jnp.int32) * tile + plane * rows + inner // capacity
    result = dot(onehot(source == iota((total, count), 1)), held_ref[...])
    for t in range(sectors * rows):
        for b in range(blocks):
            at = (t * blocks + b) * capacity
            spread_ref[at : at + capacity, :] = result[t * capacity : (t + 1) * capacity, b * 128 : (b + 1) * 128]
    out_ref[...] = spread_ref[...].astype(BF16)


def unpack_kernel(capacity, pool, cores, ids_ref, map_ref, own_ref, peer_ref, out_ref):
    core = ids_ref[2]
    tiles = map_ref.shape[1]
    width = out_ref.shape[2]
    blocks = width // 128
    owner_row = jnp.broadcast_to(map_ref[...], (tiles, tiles)) // pool
    eye = iota((tiles, tiles), 0) == iota((tiles, tiles), 1)
    owner = jnp.sum(jnp.where(eye, owner_row, 0).astype(F32), axis=1, keepdims=True).astype(jnp.int32)
    before = (owner == owner_row) & (iota((tiles, tiles), 1) < iota((tiles, tiles), 0))
    rank = jnp.sum(jnp.where(before, F32(1.0), F32(0.0)), axis=1, keepdims=True).astype(jnp.int32)
    place = (owner // cores * cores + core) * (blocks * capacity) + rank
    own = jnp.where(owner % cores == core, place, -own_ref.shape[0])
    peer = jnp.where(owner % cores == core, -own_ref.shape[0], place)
    column = iota((tiles, own_ref.shape[0]), 1)
    for b in range(blocks):
        value = dot(onehot(column == own + b * capacity), own_ref[...])
        value = value + dot(onehot(column == peer + b * capacity), peer_ref[...])
        for copy in range(out_ref.shape[0]):
            out_ref[copy, :, b * 128 : (b + 1) * 128] = value.astype(BF16)


def weight_kernel(slab, states, group, ids_ref, fields_ref, tensor_ref, mask_ref, out_ref):
    plane = ids_ref[1]
    slots, cols = tensor_ref.shape
    planes = slots // slab
    pairs = slab * states
    rows = pairs * group
    total = states * rows
    deep = slots * group
    mask = mask_ref[...].astype(BF16)
    lanes_v = onehot(iota((slots, cols), 1) // (states * states) == iota((slots, cols), 0))
    base = tensor_ref[...] * dot(mask, lanes_v)
    w = iota((slots, cols), 0)
    lane = iota((slots, cols), 1)
    q, s = lane // states, lane % states
    first = F32(0.5) - (s // 2).astype(F32)
    second = F32(0.5) - (s % 2).astype(F32)
    onsite = fields_ref[0] * first + fields_ref[1] * second
    base = base + jnp.where((w == ids_ref[3] - 1) & (q == s) & (lane < states * states), onsite, F32(0.0))
    high = base.astype(BF16)
    low = (base - high.astype(F32)).astype(BF16)
    row = iota((total, cols), 0)
    pair = (row // group) % pairs
    state = row // rows
    wanted = (plane * slab + pair // states) * (states * states) + (pair % states) * states + state
    choose = onehot(wanted == iota((total, cols), 1))
    slot = iota((slots, deep), 1) // group
    slot = (plane - slot // slab + planes) % planes * slab + slot % slab
    widen = onehot(slot == iota((slots, deep), 0))
    diagonal = iota((total, deep), 0) % group == iota((total, deep), 1) % group
    for part, value in ((0, high), (1, low)):
        tall = dot_t(choose, value).astype(BF16)
        out_ref[:, part * deep : (part + 1) * deep] = jnp.where(diagonal, dot(tall, widen), F32(0.0)).astype(BF16)


def call_weights(ids, fields, tensor, mask, slab, states):
    slots = tensor.shape[0]
    return pl.pallas_call(
        functools.partial(weight_kernel, slab, states, GROUP),
        in_specs=[SMEM] * 2 + vmem(2),
        out_specs=pl.BlockSpec(memory_space=pltpu.VMEM),
        out_shape=jax.ShapeDtypeStruct((states * slab * states * GROUP, 2 * slots * GROUP), BF16),
        cost_estimate=pl.CostEstimate(flops=1 << 28, bytes_accessed=1 << 19, transcendentals=0),
        name="weights",
    )(ids, fields, tensor, mask)


def turn_kernel(tile, ids_ref, env_ref, out_ref):
    core = ids_ref[2]
    slab, share, width = out_ref.shape
    runs = width // tile
    row = iota((share, width), 0) + core * share
    rows = onehot(row % runs * tile + row // runs == iota((share, width), 1))
    column = iota((width, width), 1)
    columns = onehot(column % runs * tile + column // runs == iota((width, width), 0))
    for w in range(slab):
        out_ref[w] = dot(dot(rows, env_ref[w]).astype(BF16), columns).astype(BF16)


def call_turn(ids, env, tile):
    slab, width, _ = env.shape
    return pl.pallas_call(
        functools.partial(turn_kernel, tile),
        in_specs=[SMEM] + vmem(1),
        out_specs=pl.BlockSpec(memory_space=pltpu.VMEM),
        out_shape=jax.ShapeDtypeStruct((slab, width // 2, width), BF16),
        cost_estimate=pl.CostEstimate(flops=1 << 28, bytes_accessed=2 << 20, transcendentals=0),
        name="turn",
    )(ids, env)


def fold_kernel(ids_ref, weight_ref, own_ref, got_ref, out_ref):
    slab, step_rows, width = own_ref.shape
    slots = slab + got_ref.shape[0]
    states = out_ref.shape[2] // width
    pairs = out_ref.shape[0]
    rows = pairs * GROUP
    for at in range(0, step_rows, 2 * GROUP):
        here = slice(at, at + 2 * GROUP)
        env = jnp.concatenate([own_ref[:, here, :], got_ref[:, here, :]], axis=0).astype(F32)
        side = [env[:, h * GROUP : (h + 1) * GROUP, :].reshape(slots * GROUP, width) for h in range(2)]
        side = jnp.concatenate(side, axis=1).astype(BF16)
        value = dot(weight_ref[...], jnp.concatenate([side, side], axis=0))
        for s in range(states):
            part = [
                value[s * rows : (s + 1) * rows, h * width : (h + 1) * width].reshape(pairs, GROUP, width)
                for h in range(2)
            ]
            out_ref[:, here, s * width : (s + 1) * width] = jnp.concatenate(part, axis=1).astype(BF16)


def apply_kernel(tile, ids_ref, kept_ref, mine_ref, twin_ref, *refs):
    folded = refs[: 2 * CHUNKS]
    out_ref, ordered, halves, own, turned = refs[2 * CHUNKS :]
    core = ids_ref[2]
    planes, tiles, width = mine_ref.shape
    states = tiles * tile // width
    per_state = tiles // states
    share = own.shape[1]

    @pl.when(pl.program_id(0) == 0)
    def _():
        keep = iota((tiles, width), 1) < kept_ref[0]
        for p in range(planes):
            for other, ref in ((0, mine_ref), (1, twin_ref)):
                ordered[p * 2 + (core + other) % 2] = jnp.where(keep, ref[p], jnp.zeros((), BF16))
        for s in range(states):
            value = ordered[:, s * per_state : (s + 1) * per_state, :].reshape(width, width).astype(F32)
            own[s * width : (s + 1) * width, :] = jnp.where(core == 0, value[:, :share], value[:, share:]).astype(BF16)
            first = pl.multiple_of(s * width + core * share, share)
            second = pl.multiple_of(s * width + (1 - core) * share, share)
            halves[pl.ds(first, share), :] = value[:share].astype(BF16)
            halves[pl.ds(second, share), :] = value[share:].astype(BF16)

    for q in range(states):
        mid = dot(jnp.concatenate([ref[q] for ref in folded], axis=0), own[...])
        turned[:, q * width : (q + 1) * width] = jnp.swapaxes(mid, 0, 1).astype(BF16)
    out_ref[0, 0] = dot(turned[...], halves[...])


def fold(ids, weights, own, got, states):
    others, count, width = got.shape
    slab = own.shape[0]
    pairs = slab * states
    step = 48
    steps = count // step
    return pl.pallas_call(
        fold_kernel,
        grid_spec=pltpu.PrefetchScalarGridSpec(
            num_scalar_prefetch=1,
            grid=(steps,),
            in_specs=[
                pl.BlockSpec(weights.shape, lambda i, ids: (0, 0)),
                pl.BlockSpec((slab, step, width), lambda i, ids: (0, i, 0)),
                pl.BlockSpec((others, step, width), lambda i, ids: (0, i, 0)),
            ],
            out_specs=pl.BlockSpec((pairs, step, states * width), lambda i, ids: (0, i, 0)),
        ),
        out_shape=jax.ShapeDtypeStruct((pairs, count, states * width), BF16),
        cost_estimate=pl.CostEstimate(flops=2 * count * 64 * 256 * width, bytes_accessed=6 << 20, transcendentals=0),
    )(ids, weights, own, got)


def call_pack(ids, owner_map, held, capacity, tile, rows):
    sectors, width = owner_map.shape[0], held.shape[1]
    count = sectors * rows * capacity * width // 128
    return pl.pallas_call(
        functools.partial(pack_kernel, capacity, tile, rows),
        in_specs=[SMEM] + vmem(2),
        out_specs=pl.BlockSpec(memory_space=pltpu.VMEM),
        out_shape=jax.ShapeDtypeStruct((count, 128), BF16),
        scratch_shapes=[pltpu.VMEM((count, 128), F32)],
        cost_estimate=pl.CostEstimate(flops=1 << 29, bytes_accessed=2 << 20, transcendentals=0),
        name="pack",
    )(ids, owner_map, held)


def call_unpack(ids, map_here, arrived, swapped, capacity, pool, cores, copies):
    tiles = map_here.shape[1]
    width = arrived.size // tiles // 2
    return pl.pallas_call(
        functools.partial(unpack_kernel, capacity, pool, cores),
        in_specs=[SMEM] + vmem(3),
        out_specs=pl.BlockSpec(memory_space=pltpu.VMEM),
        out_shape=jax.ShapeDtypeStruct((copies, tiles, width), BF16),
        cost_estimate=pl.CostEstimate(flops=1 << 28, bytes_accessed=2 << 20, transcendentals=0),
        compiler_params=pltpu.CompilerParams(vmem_limit_bytes=16 << 20),
        name="unpack",
    )(ids, map_here, arrived, swapped)


def call_apply(ids, kept, by_plane, by_twin, folded, tile):
    planes, tiles, width = by_plane.shape
    pairs, part, deep = folded[0].shape
    share = width // 2
    states = deep // width
    slab = pairs // states
    whole = lambda v, *_: (0, 0, 0)
    return pl.pallas_call(
        functools.partial(apply_kernel, tile),
        grid_spec=pltpu.PrefetchScalarGridSpec(
            num_scalar_prefetch=2,
            grid=(slab,),
            in_specs=[pl.BlockSpec((planes, tiles, width), whole)] * 2
            + [pl.BlockSpec((states, part, deep), lambda v, *_: (v, 0, 0))] * len(folded),
            out_specs=pl.BlockSpec((1, 1, share, width), lambda v, *_: (v, 0, 0, 0)),
            scratch_shapes=[
                pltpu.VMEM((tile, tiles, width), BF16),
                pltpu.VMEM((deep, width), BF16),
                pltpu.VMEM((deep, share), BF16),
                pltpu.VMEM((share, deep), BF16),
            ],
        ),
        out_shape=jax.ShapeDtypeStruct((slab, 1, share, width), F32),
        cost_estimate=pl.CostEstimate(flops=9 << 29, bytes_accessed=22 << 20, transcendentals=0),
        name="apply",
    )(ids, kept, by_plane, by_twin, *folded)


def on_device(held, owner_map, kept, left_env, mpo_tensor, mpo_mask, fields):
    env_count = lax.axis_size("env")
    cores = lax.axis_size("col")
    planes = lax.axis_size("mpo")
    env_row = lax.axis_index("env")
    core = lax.axis_index("col")
    plane = lax.axis_index("mpo")
    pool, tile, width = held.shape
    tiles = owner_map.shape[1]
    states = tiles * tile // width
    capacity = 2 * tiles // (env_count * cores)
    rows = tile // planes
    slab = left_env.shape[0]
    slots = slab * planes
    bond = mpo_tensor.shape[0]
    ids = jnp.stack([env_row * cores + core, plane, core, jnp.int32(bond)]).astype(jnp.int32)

    def twin(x):
        return lax.ppermute(x, "col", [(0, 1), (1, 0)])

    message = rows * capacity * width // 128
    packed = call_pack(ids, owner_map, held.reshape(pool * tile, width), capacity, tile, rows)
    arrived = lax.all_to_all(packed.reshape(env_count, message // 4, 4, 128), "env", 0, 0, tiled=True)

    env_own = left_env[:, 0]
    step = lambda x, d: lax.ppermute(x, "mpo", [(i, (i + d) % planes) for i in range(planes)])
    ring = [(i * cores + c, (i + 1 - 2 * c) % planes * cores + c) for i in range(planes) for c in range(cores)]
    part = call_turn(ids, env_own, tile)
    from_left, from_right = step(part, 1), step(part, -1)
    tensor = jnp.pad(
        mpo_tensor.reshape(bond, bond * states * states), ((0, slots - bond), (0, (slots - bond) * states * states))
    )
    mask = jnp.pad(mpo_mask.astype(F32), ((0, slots - bond), (0, slots - bond)))
    weights = call_weights(ids, fields, tensor, mask, slab, states)
    map_here = lax.dynamic_slice_in_dim(owner_map, env_row, 1, 0)
    onward = jnp.where(core == 0, from_left, from_right)
    onward, weights, map_here = lax.optimization_barrier((onward, weights, map_here))
    from_far = lax.ppermute(onward, ("mpo", "col"), ring)
    env_got = jnp.concatenate([from_left, from_far, from_right], axis=0)
    part_twin = twin(part)
    env_twin = twin(env_got)
    folded = []
    for own, got in ((part, env_got), (part_twin, env_twin)):
        folded.append(fold(ids, weights, own, got, states))

    arrived = arrived.reshape(env_count * message, 128)
    swapped = twin(arrived)
    mine = call_unpack(ids, map_here, arrived, swapped, capacity, pool, cores, planes)
    by_plane = lax.all_to_all(mine, "mpo", 0, 0, tiled=True)
    by_twin = twin(by_plane)
    result = call_apply(ids, kept, by_plane, by_twin, folded, tile)
    return jnp.swapaxes(result, 2, 3)


def solution(mesh):
    return jax.shard_map(
        on_device,
        mesh=mesh,
        in_specs=(
            P(("real", "env", "col"), None, None),
            P("real", None),
            P(("real", "env")),
            P("mpo", ("real", "env"), None, None),
            P(),
            P(),
            P("real"),
        ),
        out_specs=P("mpo", ("real", "env"), None, "col"),
        check_vma=False,
    )
```

```python
import functools

import jax
import jax.numpy as jnp
from jax import lax
from jax.experimental import pallas as pl
from jax.experimental.pallas import tpu as pltpu
from jax.sharding import PartitionSpec as P


F32 = jnp.float32
BF16 = jnp.bfloat16


GROUP = 8


def iota(shape, dim):
    return lax.broadcasted_iota(jnp.int32, shape, dim)


def onehot(condition):
    return jnp.where(condition, F32(1.0), F32(0.0)).astype(BF16)


def dot(a, b):
    return lax.dot_general(a, b, (((1,), (0,)), ((), ())), preferred_element_type=F32)


def dot_t(a, b):
    return lax.dot_general(a, b, (((1,), (1,)), ((), ())), preferred_element_type=F32)


def vmem(n):
    return [pl.BlockSpec(memory_space=pltpu.VMEM)] * n


SMEM = pl.BlockSpec(memory_space=pltpu.SMEM)


def pack_kernel(capacity, tile, rows, ids_ref, map_ref, held_ref, out_ref, spread_ref):
    me, plane = ids_ref[0], ids_ref[1]
    sectors, tiles = map_ref.shape
    count, width = held_ref.shape
    pool = count // tile
    blocks = width // 128
    local = map_ref[...] - me * pool
    mine = (local >= 0) & (local < pool)
    upto = onehot(iota((tiles, tiles), 0) <= iota((tiles, tiles), 1))
    rank = dot(onehot(mine), upto)
    slots = jnp.zeros((sectors, 128), F32)
    lane = iota((sectors, 128), 1)
    for s in range(capacity):
        hit = mine & (rank == F32(s + 1))
        value = jnp.sum(jnp.where(hit, local, 0).astype(F32), axis=1, keepdims=True)
        slots = slots + jnp.where(lane == s, value, F32(0.0))
    group = capacity * rows
    total = sectors * group
    inner = iota((total, 1), 0) % group
    sector = iota((total, sectors), 0) // group
    spread = dot(onehot(sector == iota((total, sectors), 1)), slots.astype(BF16))
    slot = jnp.sum(jnp.where(iota((total, 128), 1) == inner % capacity, spread, F32(0.0)), axis=1, keepdims=True)
    source = slot.astype(jnp.int32) * tile + plane * rows + inner // capacity
    result = dot(onehot(source == iota((total, count), 1)), held_ref[...])
    for t in range(sectors * rows):
        for b in range(blocks):
            at = (t * blocks + b) * capacity
            spread_ref[at : at + capacity, :] = result[t * capacity : (t + 1) * capacity, b * 128 : (b + 1) * 128]
    out_ref[...] = spread_ref[...].astype(BF16)


def unpack_kernel(capacity, pool, cores, ids_ref, map_ref, own_ref, peer_ref, out_ref):
    core = ids_ref[2]
    tiles = map_ref.shape[1]
    width = out_ref.shape[2]
    blocks = width // 128
    owner_row = jnp.broadcast_to(map_ref[...], (tiles, tiles)) // pool
    eye = iota((tiles, tiles), 0) == iota((tiles, tiles), 1)
    owner = jnp.sum(jnp.where(eye, owner_row, 0).astype(F32), axis=1, keepdims=True).astype(jnp.int32)
    before = (owner == owner_row) & (iota((tiles, tiles), 1) < iota((tiles, tiles), 0))
    rank = jnp.sum(jnp.where(before, F32(1.0), F32(0.0)), axis=1, keepdims=True).astype(jnp.int32)
    place = (owner // cores * cores + core) * (blocks * capacity) + rank
    own = jnp.where(owner % cores == core, place, -own_ref.shape[0])
    peer = jnp.where(owner % cores == core, -own_ref.shape[0], place)
    column = iota((tiles, own_ref.shape[0]), 1)
    for b in range(blocks):
        value = dot(onehot(column == own + b * capacity), own_ref[...])
        value = value + dot(onehot(column == peer + b * capacity), peer_ref[...])
        for copy in range(out_ref.shape[0]):
            out_ref[copy, :, b * 128 : (b + 1) * 128] = value.astype(BF16)


def weight_kernel(slab, states, group, ids_ref, fields_ref, tensor_ref, mask_ref, out_ref):
    plane = ids_ref[1]
    slots, cols = tensor_ref.shape
    planes = slots // slab
    pairs = slab * states
    rows = pairs * group
    total = states * rows
    deep = slots * group
    mask = mask_ref[...].astype(BF16)
    lanes_v = onehot(iota((slots, cols), 1) // (states * states) == iota((slots, cols), 0))
    base = tensor_ref[...] * dot(mask, lanes_v)
    w = iota((slots, cols), 0)
    lane = iota((slots, cols), 1)
    q, s = lane // states, lane % states
    first = F32(0.5) - (s // 2).astype(F32)
    second = F32(0.5) - (s % 2).astype(F32)
    onsite = fields_ref[0] * first + fields_ref[1] * second
    base = base + jnp.where((w == ids_ref[3] - 1) & (q == s) & (lane < states * states), onsite, F32(0.0))
    high = base.astype(BF16)
    low = (base - high.astype(F32)).astype(BF16)
    row = iota((total, cols), 0)
    pair = (row // group) % pairs
    state = row // rows
    wanted = (plane * slab + pair // states) * (states * states) + (pair % states) * states + state
    choose = onehot(wanted == iota((total, cols), 1))
    slot = iota((slots, deep), 1) // group
    slot = (plane - slot // slab + planes) % planes * slab + slot % slab
    widen = onehot(slot == iota((slots, deep), 0))
    diagonal = iota((total, deep), 0) % group == iota((total, deep), 1) % group
    for part, value in ((0, high), (1, low)):
        tall = dot_t(choose, value).astype(BF16)
        out_ref[:, part * deep : (part + 1) * deep] = jnp.where(diagonal, dot(tall, widen), F32(0.0)).astype(BF16)


def call_weights(ids, fields, tensor, mask, slab, states):
    slots = tensor.shape[0]
    return pl.pallas_call(
        functools.partial(weight_kernel, slab, states, GROUP),
        in_specs=[SMEM] * 2 + vmem(2),
        out_specs=pl.BlockSpec(memory_space=pltpu.VMEM),
        out_shape=jax.ShapeDtypeStruct((states * slab * states * GROUP, 2 * slots * GROUP), BF16),
        cost_estimate=pl.CostEstimate(flops=1 << 28, bytes_accessed=1 << 19, transcendentals=0),
        name="weights",
    )(ids, fields, tensor, mask)


def fold_kernel(ids_ref, weight_ref, own_ref, got_ref, out_ref):
    slab, step_rows, width = own_ref.shape
    slots = slab + got_ref.shape[0]
    states = out_ref.shape[2] // width
    pairs = out_ref.shape[0]
    rows = pairs * GROUP
    for at in range(0, step_rows, 2 * GROUP):
        here = slice(at, at + 2 * GROUP)
        env = jnp.concatenate([own_ref[:, here, :], got_ref[:, here, :]], axis=0).astype(F32)
        side = [env[:, h * GROUP : (h + 1) * GROUP, :].reshape(slots * GROUP, width) for h in range(2)]
        side = jnp.concatenate(side, axis=1).astype(BF16)
        value = dot(weight_ref[...], jnp.concatenate([side, side], axis=0))
        for s in range(states):
            part = [
                value[s * rows : (s + 1) * rows, h * width : (h + 1) * width].reshape(pairs, GROUP, width)
                for h in range(2)
            ]
            out_ref[:, here, s * width : (s + 1) * width] = jnp.concatenate(part, axis=1).astype(BF16)


def apply_kernel(tile, ids_ref, kept_ref, rows_ref, *refs):
    folded = refs[:-4]
    out_ref, halves, own, turned = refs[-4:]
    core = ids_ref[2]
    _, tiles, width = rows_ref.shape
    states = tiles * tile // width
    per_state = tiles // states
    share = own.shape[1]

    @pl.when(pl.program_id(0) == 0)
    def _():
        keep = iota((width, width), 1) < kept_ref[0]
        n, k = iota((width, width), 0), iota((width, width), 1)
        turn = onehot((n % tile) * per_state + n // tile == k)
        for s in range(states):
            mixed = rows_ref[:, s * per_state : (s + 1) * per_state, :].reshape(width, width)
            value = jnp.where(keep, dot(turn, mixed), F32(0.0))
            own[s * width : (s + 1) * width, :] = jnp.where(core == 0, value[:, :share], value[:, share:]).astype(BF16)
            first = pl.multiple_of(s * width + core * share, share)
            second = pl.multiple_of(s * width + (1 - core) * share, share)
            halves[pl.ds(first, share), :] = value[:share].astype(BF16)
            halves[pl.ds(second, share), :] = value[share:].astype(BF16)

    for q in range(states):
        mid = dot(jnp.concatenate([ref[q] for ref in folded], axis=0), own[...])
        turned[:, q * width : (q + 1) * width] = jnp.swapaxes(mid, 0, 1).astype(BF16)
    out_ref[0, 0] = dot(turned[...], halves[...])


def fold(ids, weights, own, got, half, begin, count, states):
    others, share, width = got.shape
    slab = own.shape[0]
    pairs = slab * states
    step = 48
    first, whole = begin // step, share // step
    return pl.pallas_call(
        fold_kernel,
        grid_spec=pltpu.PrefetchScalarGridSpec(
            num_scalar_prefetch=1,
            grid=(count // step,),
            in_specs=[
                pl.BlockSpec(weights.shape, lambda i, ids: (0, 0)),
                pl.BlockSpec((slab, step, width), lambda i, ids: (0, (ids[2] + half) % 2 * whole + first + i, 0)),
                pl.BlockSpec((others, step, width), lambda i, ids: (0, first + i, 0)),
            ],
            out_specs=pl.BlockSpec((pairs, step, states * width), lambda i, ids: (0, i, 0)),
        ),
        out_shape=jax.ShapeDtypeStruct((pairs, count, states * width), BF16),
        cost_estimate=pl.CostEstimate(flops=2 * count * 64 * 256 * width, bytes_accessed=6 << 20, transcendentals=0),
    )(ids, weights, own, got)


def call_pack(ids, owner_map, held, capacity, tile, rows):
    sectors, width = owner_map.shape[0], held.shape[1]
    count = sectors * rows * capacity * width // 128
    return pl.pallas_call(
        functools.partial(pack_kernel, capacity, tile, rows),
        in_specs=[SMEM] + vmem(2),
        out_specs=pl.BlockSpec(memory_space=pltpu.VMEM),
        out_shape=jax.ShapeDtypeStruct((count, 128), BF16),
        scratch_shapes=[pltpu.VMEM((count, 128), F32)],
        cost_estimate=pl.CostEstimate(flops=1 << 29, bytes_accessed=2 << 20, transcendentals=0),
        name="pack",
    )(ids, owner_map, held)


def call_unpack(ids, map_here, arrived, swapped, capacity, pool, cores, copies):
    tiles = map_here.shape[1]
    width = arrived.size // tiles // 2
    return pl.pallas_call(
        functools.partial(unpack_kernel, capacity, pool, cores),
        in_specs=[SMEM] + vmem(3),
        out_specs=pl.BlockSpec(memory_space=pltpu.VMEM),
        out_shape=jax.ShapeDtypeStruct((copies, tiles, width), BF16),
        cost_estimate=pl.CostEstimate(flops=1 << 28, bytes_accessed=2 << 20, transcendentals=0),
        compiler_params=pltpu.CompilerParams(vmem_limit_bytes=16 << 20),
        name="unpack",
    )(ids, map_here, arrived, swapped)


def call_apply(ids, kept, rows, folded, tile):
    _, tiles, width = rows.shape
    pairs, _, deep = folded[0].shape
    share = width // 2
    states = deep // width
    slab = pairs // states
    whole = lambda v, *_: (0, 0, 0)
    return pl.pallas_call(
        functools.partial(apply_kernel, tile),
        grid_spec=pltpu.PrefetchScalarGridSpec(
            num_scalar_prefetch=2,
            grid=(slab,),
            in_specs=[pl.BlockSpec((tile, tiles, width), whole)]
            + [pl.BlockSpec((states, part.shape[1], deep), lambda v, *_: (v, 0, 0)) for part in folded],
            out_specs=pl.BlockSpec((1, 1, share, width), lambda v, *_: (v, 0, 0, 0)),
            scratch_shapes=[
                pltpu.VMEM((deep, width), BF16),
                pltpu.VMEM((deep, share), BF16),
                pltpu.VMEM((share, deep), BF16),
            ],
        ),
        out_shape=jax.ShapeDtypeStruct((slab, 1, share, width), F32),
        cost_estimate=pl.CostEstimate(flops=9 << 29, bytes_accessed=22 << 20, transcendentals=0),
        name="apply",
    )(ids, kept, rows, *folded)


def on_device(held, owner_map, kept, left_env, mpo_tensor, mpo_mask, fields):
    env_count = lax.axis_size("env")
    cores = lax.axis_size("col")
    planes = lax.axis_size("mpo")
    env_row = lax.axis_index("env")
    core = lax.axis_index("col")
    plane = lax.axis_index("mpo")
    pool, tile, width = held.shape
    tiles = owner_map.shape[1]
    states = tiles * tile // width
    capacity = 2 * tiles // (env_count * cores)
    rows = tile // planes
    slab = left_env.shape[0]
    slots = slab * planes
    bond = mpo_tensor.shape[0]
    ids = jnp.stack([env_row * cores + core, plane, core, jnp.int32(bond)]).astype(jnp.int32)

    def twin(x):
        return lax.ppermute(x, "col", [(0, 1), (1, 0)])

    message = rows * capacity * width // 128
    packed = call_pack(ids, owner_map, held.reshape(pool * tile, width), capacity, tile, rows)
    arrived = lax.all_to_all(packed.reshape(env_count, message // 4, 4, 128), "env", 0, 0, tiled=True)

    share = width // cores
    env_own = left_env[:, 0]
    step = lambda x, d: lax.ppermute(x, "mpo", [(i, (i + d) % planes) for i in range(planes)])
    ring = [(i * cores + c, (i + 1 - 2 * c) % planes * cores + c) for i in range(planes) for c in range(cores)]
    part = lax.dynamic_slice_in_dim(env_own, core * share, share, 1)
    from_left, from_right = step(part, 1), step(part, -1)
    tensor = jnp.pad(
        mpo_tensor.reshape(bond, bond * states * states), ((0, slots - bond), (0, (slots - bond) * states * states))
    )
    mask = jnp.pad(mpo_mask.astype(F32), ((0, slots - bond), (0, slots - bond)))
    weights = call_weights(ids, fields, tensor, mask, slab, states)
    map_here = lax.dynamic_slice_in_dim(owner_map, env_row, 1, 0)
    onward = jnp.where(core == 0, from_left, from_right)
    onward, weights, map_here = lax.optimization_barrier((onward, weights, map_here))
    from_far = lax.ppermute(onward, ("mpo", "col"), ring)
    env_got = jnp.concatenate([from_left, from_far, from_right], axis=0)
    env_twin = twin(env_got)
    folded = []
    early = share // 2
    for half, got, begin, count in (
        (0, env_got, 0, early), (0, env_got, early, share - early), (1, env_twin, 0, share)
    ):
        folded.append(fold(ids, weights, env_own, got, half, begin, count, states))

    arrived = arrived.reshape(env_count * message, 128)
    swapped = twin(arrived)
    mine = call_unpack(ids, map_here, arrived, swapped, capacity, pool, cores, planes * cores)
    tile_rows = lax.all_to_all(mine, ("mpo", "col"), 0, 0, tiled=True)
    result = call_apply(ids, kept, tile_rows, folded, tile)
    return jnp.swapaxes(result, 2, 3)


def solution(mesh):
    return jax.shard_map(
        on_device,
        mesh=mesh,
        in_specs=(
            P(("real", "env", "col"), None, None),
            P("real", None),
            P(("real", "env")),
            P("mpo", ("real", "env"), None, None),
            P(),
            P(),
            P("real"),
        ),
        out_specs=P("mpo", ("real", "env"), None, "col"),
        check_vma=False,
    )
```
